256 devices in a mesh: tm: 128 (over y_hi, z, x, core), mom: 2 (over y_lo).
Axes of the slice: x: 4, y: 4 (y_hi: 2, y_lo: 2; y = y_hi * 2 + y_lo), z: 8, core: 2. Of those that a mesh axis runs over, the one named last changes fastest.
Arguments:
- fields: bfloat16 [128, 4, 2, 512, 512], P('tm', 'mom'), may hold values from -1 to 1
- mom_pairs: int32 [6, 2], P('mom'), may hold values from 0 to 3, as said below
- deltas: int32 [4], replicated, may hold values from 0 to 3, each once
Outputs:
- time_traces: float32 [128, 2, 4, 6], P('tm', None, None, 'mom')
- summed_traces: float32 [2, 4, 6], P(None, None, 'mom')
The draws below stay inside these ranges and needn't reach their ends.
Inputs may be any that keep to these rules, and one draw needn't show every extreme that they name: `mom_pairs`: column 0 may be any momentum; in row r, column 1 lies in momentum group r // 3, that is from (r // 3) * 2 to (r // 3) * 2 + 1.
All inputs are finite; a program needn't handle non-finite values.
Results may differ from the reference program's by a relative error of at most 0.0003.
Values may be sent and summed in bfloat16 or wider, within the bound.
A program may use at most 128 MiB of HBM per device.

```python
import jax
import jax.numpy as jnp
from jax import lax

NEV = 512
PG = 2
PAIR_DEV = 3
NSEP = 4
P_SIZE = 4
NPAIR = 6
NT = 128


def draw_fields(key, part):
    field_shape = (NT, P_SIZE, 2, NEV, NEV)
    key_base = jax.random.fold_in(jax.random.fold_in(key, 11), 0)
    growth = jnp.sqrt(3.0) ** (jnp.arange(NT, dtype=jnp.float32) / max(NT - 1, 1))
    values = jax.random.normal(key_base, field_shape, jnp.float32)
    values = values * growth[:, None, None, None, None] / jnp.sqrt(jnp.float32(NEV))
    return jnp.clip(values, -1.0, 1.0).astype(jnp.bfloat16)


def draw_mom_pairs(key, part):
    key_source, key_target = jax.random.split(jax.random.fold_in(key, 23), 2)
    source_mom = jax.random.randint(key_source, (NPAIR,), 0, P_SIZE)
    owner = jnp.arange(NPAIR, dtype=jnp.int32) // PAIR_DEV
    target_mom = owner * PG + jax.random.randint(key_target, (NPAIR,), 0, PG)
    return jnp.stack([source_mom, target_mom], axis=1).astype(jnp.int32)


def setup_inputs(seed: int = 0) -> dict:
    streams_of = jax.random.split(jax.random.key(seed), 4)
    fields = draw_fields(jax.random.fold_in(streams_of[3], 71), 0)
    mom_pairs = draw_mom_pairs(jax.random.fold_in(streams_of[3], 71), 0)
    deltas = jax.random.permutation(streams_of[2], NSEP).astype(jnp.int32)
    return dict(fields=fields, mom_pairs=mom_pairs, deltas=deltas)


def products(source, target):
    product_full = jnp.einsum("xij,yjk->xyik", source.astype(jnp.float32), target.astype(jnp.float32))
    real_part = product_full[0, 0] - product_full[1, 1]
    imag_part = product_full[0, 1] + product_full[1, 0]
    direct = jnp.trace(real_part)
    box_value = jnp.sum(real_part * real_part.T) - jnp.sum(imag_part * imag_part.T)
    return direct, box_value


def reference(fields, mom_pairs, deltas):
    slices = fields.shape[0]
    pair_count = mom_pairs.shape[0]

    def one_time(time_slice):
        source_slice = lax.dynamic_index_in_dim(fields, time_slice, 0, keepdims=False)
        per_sep = []
        for separation in range(1, NSEP + 1):
            later = ((time_slice + separation) % slices).astype(jnp.int32)
            target_slice = lax.dynamic_index_in_dim(fields, later, 0, keepdims=False)
            directs = []
            boxes = []
            for which in range(pair_count):
                source = lax.dynamic_index_in_dim(source_slice, mom_pairs[which, 0].astype(jnp.int32), 0, keepdims=False)
                target = lax.dynamic_index_in_dim(target_slice, mom_pairs[which, 1].astype(jnp.int32), 0, keepdims=False)
                direct, box_value = products(source, target)
                directs.append(direct)
                boxes.append(box_value)
            per_sep.append(jnp.stack([jnp.stack(directs), jnp.stack(boxes)]))
        return jnp.stack(per_sep, axis=1)

    stacked = lax.map(one_time, jnp.arange(slices, dtype=jnp.int32))
    time_traces = jnp.take(stacked, deltas.astype(jnp.int32), axis=2)
    summed_traces = jnp.sum(time_traces, axis=0)
    return time_traces, summed_traces
```

```python
import functools

import jax
import jax.numpy as jnp
from jax import lax
from jax.experimental import pallas as pl
from jax.experimental.pallas import tpu as pltpu
from jax.sharding import PartitionSpec as P

MESH = pl.DeviceIdType.MESH
CHIPS_PER_PLANE = 32
ROWS = 128
CHUNKS = 4
SUB = 4
PIECES = CHUNKS * SUB
PIECE_ROWS = ROWS // SUB
NEV = ROWS * CHUNKS
PAIRS = 3
SEPS = 4


def place():
    time, group = lax.axis_index("tm"), lax.axis_index("mom")
    count = lax.axis_size("tm")
    chip, core = time // 2, time % 2
    swap_right = (chip % CHIPS_PER_PLANE) // (CHIPS_PER_PLANE - 1)
    swap_left = ((chip + 1) % CHIPS_PER_PLANE == 1).astype(jnp.int32)
    right = {"tm": (time + 2) % count, "mom": (group + swap_right) % 2}
    left = {"tm": (time + count - 2) % count, "mom": (group + swap_left) % 2}
    across = {"tm": time, "mom": 1 - group}
    partner = {"tm": time + 1 - 2 * core, "mom": group}
    return time, group, core, right, left, across, partner


def folded(values):
    total = values.reshape(-1, 8, values.shape[-1]).sum(0)
    lanes = [total[:, i : i + 128] for i in range(0, values.shape[-1], 128)]
    return functools.reduce(jnp.add, lanes)


def trace_kernel(
    pairs_own, pairs_sent, fields, tile,
    own, near, fed, ahead, source, wide, sums, flips, boxes, directs, rows_out, pairs_in, pairs_other,
    load_sem, pair_sems, near_sems, send_right, recv_right, send_left, recv_left, send_y, recv_y, send_core, recv_core,
):
    time, group, core, right, left, across, partner = place()
    from_left = left["mom"]
    from_right = right["mom"]

    def rows(j):
        return pl.ds(pl.multiple_of(j * PIECE_ROWS, PIECE_ROWS), PIECE_ROWS)

    def remote(src, dst, send, recv, device):
        return pltpu.make_async_remote_copy(
            src_ref=src, dst_ref=dst, send_sem=send, recv_sem=recv, device_id=device, device_id_type=MESH
        )

    def to_right(j):
        return remote(
            own.at[:, :, rows(j), :], source.at[group, :, :, rows(j), :], send_right.at[j], recv_right.at[j], right
        )

    def to_left(j):
        return remote(own.at[:, :, rows(j), :], ahead.at[:, :, rows(j), :], send_left.at[j], recv_left.at[j], left)

    def over_y(j):
        part = source.at[from_left, :, :, rows(j), :]
        return remote(part, part, send_y.at[j], recv_y.at[j], across)

    def feed_source(j):
        return remote(
            source.at[from_left, :, :, rows(j), :], fed.at[:, :, rows(j), :], send_core.at[j], recv_core.at[j], partner
        )

    def feed_ahead(j):
        return remote(ahead.at[:, :, rows(j), :], fed.at[:, :, rows(j), :], send_core.at[j], recv_core.at[j], partner)

    near_copy = remote(own, near, near_sems.at[0], near_sems.at[1], partner)
    pair_copy = remote(pairs_sent, pairs_in, pair_sems.at[0], pair_sems.at[1], across)
    load = pltpu.make_async_copy(fields, own, load_sem)

    barrier = pltpu.get_barrier_semaphore()
    load.start()
    for device in (right, left, across, partner):
        pl.semaphore_signal(barrier, inc=1, device_id=device, device_id_type=MESH)
    load.wait()
    pl.semaphore_wait(barrier, 4)

    @pl.when(core == 1)
    def _():
        @pl.loop(0, PIECES)
        def _(j):
            to_right(j).start()

    @pl.when(core == 0)
    def _():
        @pl.loop(0, PIECES)
        def _(j):
            to_left(j).start()

    pair_copy.start()
    near_copy.start()

    @pl.loop(0, SEPS * PAIRS)
    def _(i):
        boxes[i] = jnp.zeros((8, 128), jnp.float32)
        directs[i] = jnp.zeros((8, 128), jnp.float32)

        @pl.loop(0, NEV // 32)
        def _(r):
            at = pl.ds(pl.multiple_of(r * 32, 32), 32)
            sums[i, at, :] = jnp.zeros((32, NEV), jnp.float32)
            flips[i, at, :] = jnp.zeros((32, NEV), jnp.float32)

    rows_out[...] = jnp.zeros_like(rows_out)
    pair_copy.wait_recv()
    pair_load = pltpu.make_async_copy(pairs_in, pairs_other, load_sem)
    pair_load.start()
    pair_load.wait()

    @pl.when(core == 0)
    def _():
        @pl.loop(0, PIECES)
        def _(j):
            to_left(j).wait_recv()
            feed_ahead(j).start()

        @pl.loop(0, PIECES)
        def _(j):
            to_right(j).start()

    def pair(of_group, which, side):
        return jnp.where(of_group == group, pairs_own[which, side], pairs_other[which, side])

    def widen(n):
        at = pl.ds(pl.multiple_of(n * ROWS, ROWS), ROWS)
        for momentum in range(4):
            real = source[momentum // 2, momentum % 2, 0, at, :]
            imag = source[momentum // 2, momentum % 2, 1, at, :]
            wide[momentum, n, :ROWS, :NEV] = real
            wide[momentum, n, :ROWS, NEV:] = -imag
            wide[momentum, n, ROWS:, :NEV] = imag
            wide[momentum, n, ROWS:, NEV:] = real

    def work(slot, target, of_group, n):
        at = pl.ds(pl.multiple_of(n * ROWS, ROWS), ROWS)
        diagonal = (
            lax.broadcasted_iota(jnp.int32, (ROWS, NEV), 0) + n * ROWS
            == lax.broadcasted_iota(jnp.int32, (ROWS, NEV), 1)
        )
        for which in range(PAIRS):
            i = slot * PAIRS + which
            a = pair(of_group, which, 0)
            b = lax.rem(pair(of_group, which, 1), 2)
            full = jnp.dot(
                wide[a, n], target[b].reshape(2 * NEV, NEV), preferred_element_type=jnp.float32
            )
            real, imag = full[:ROWS], full[ROWS:]
            plus = real + imag
            flipped = (real - imag).T
            box = folded(plus * flips[i, at, :])
            sums[i, at, :] = plus
            flips[i, :, at] = flipped
            boxes[i] += box + folded(sums[i, :, at] * flipped)
            directs[i] += folded(jnp.where(diagonal, real, 0.0))

    @pl.loop(0, 3 * CHUNKS + 1)
    def _(step):
        for q in range(SUB):

            @pl.when(step < CHUNKS)
            def _():
                j = step * SUB + q
                to_right(j).wait_recv()
                over_y(j).start()

                @pl.when(core == 1)
                def _():
                    feed_source(j).start()

            if q == SUB - 1:

                @pl.when((step == CHUNKS - 1) & (core == 1))
                def _():
                    @pl.loop(0, PIECES)
                    def _(j):
                        to_left(j).start()

            first = (step >= 1) & (step <= CHUNKS)
            if q == 0:

                @pl.when(first)
                def _():
                    for piece in range(SUB):
                        over_y((step - 1) * SUB + piece).wait_recv()
                    widen(step - 1)
                    work(0, own, group, step - 1)

            if q == 1:

                @pl.when(step == 1)
                def _():
                    near_copy.wait_recv()

                @pl.when(first)
                def _():
                    work(1, near, group, step - 1)

            if q == 2:
                begin = 1 + core * CHUNKS

                @pl.when(step == begin)
                def _():
                    @pl.loop(0, PIECES)
                    def _(j):
                        feed_ahead(j).wait_recv()

                @pl.when((step >= begin) & (step < begin + CHUNKS))
                def _():
                    work(2, fed, jnp.where(core == 0, from_left, from_right), step - begin)

            if q == 3:
                begin = 1 + core * 2 * CHUNKS

                @pl.when((step == begin) & (core == 1))
                def _():
                    @pl.loop(0, PIECES)
                    def _(j):
                        to_left(j).wait_recv()

                @pl.when((step >= begin) & (step < begin + CHUNKS))
                def _():
                    work(3, ahead, from_right, step - begin)

    @pl.loop(0, PIECES)
    def _(j):
        to_right(j).wait_send()
        to_left(j).wait_send()
        over_y(j).wait_send()
        feed_ahead(j).wait_send()

    near_copy.wait_send()
    pair_copy.wait_send()

    separations = (1, 2 - 2 * core, 2 * core, 3)
    groups = (group, group, jnp.where(core == 0, from_left, from_right), from_right)
    for slot in range(SEPS):
        for kind, values in enumerate((directs, boxes)):
            for which in range(PAIRS):
                row = ((groups[slot] * 2 + kind) * SEPS + separations[slot]) * PAIRS + which
                rows_out[pl.ds(row, 1), :] = values[slot * PAIRS + which].sum(0, keepdims=True)
    lanes = jnp.broadcast_to(rows_out[...].sum(1, keepdims=True), (128, 128)).T
    tile[...] = lanes[:8]


def sum_kernel(
    tile, times, total, back, first, second, third, after_first, after_second,
    back_send, back_recv, send_1, recv_1, send_2, recv_2, send_3, recv_3,
):
    time, group = lax.axis_index("tm"), lax.axis_index("mom")
    count = lax.axis_size("tm")
    row, level, plane = time % 8, time // 8 % 8, time // 64
    before, behind = (time + count - 2) % count, (time + 2) % count
    in_row = [(row + d) % 8 for d in range(1, 8)]
    in_column = [(level + d) % 8 for d in range(1, 8)]
    corner = plane * 2 + group
    in_plane = [(corner + d) % 4 for d in range(1, 4)]
    row_devices = [{"tm": time - row + r, "mom": group} for r in in_row]
    column_devices = [{"tm": time + (r - level) * 8, "mom": group} for r in in_column]
    plane_devices = [{"tm": time + (r // 2 - plane) * 64, "mom": r % 2} for r in in_plane]
    back_devices = [{"tm": before, "mom": h} for h in range(2)]

    barrier = pltpu.get_barrier_semaphore()
    greeted = row_devices + column_devices + plane_devices + back_devices + [{"tm": behind, "mom": h} for h in range(2)]
    for device in greeted:
        pl.semaphore_signal(barrier, inc=1, device_id=device, device_id_type=MESH)
    pl.semaphore_wait(barrier, len(greeted))

    def remote(src, dst, send, recv, device):
        return pltpu.make_async_remote_copy(
            src_ref=src, dst_ref=dst, send_sem=send, recv_sem=recv, device_id=device, device_id_type=MESH
        )

    returns = [
        remote(tile, back.at[group], back_send.at[h], back_recv.at[group], device)
        for h, device in enumerate(back_devices)
    ]
    for copy in returns:
        copy.start()

    def stage(src, held, mine, places, devices, send, recv):
        copies = [
            remote(src, held.at[mine], send.at[d], recv.at[mine], device) for d, device in enumerate(devices)
        ]
        for copy in copies:
            copy.start()
        held[mine] = src[...]
        for d, place_of in enumerate(places):
            remote(src, held.at[place_of], send.at[d], recv.at[place_of], devices[d]).wait_recv()
        value = functools.reduce(jnp.add, [held[i] for i in range(held.shape[0])])
        return copies, value

    copies_1, value = stage(tile, first, row, in_row, row_devices, send_1, recv_1)
    after_first[...] = value
    copies_2, value = stage(after_first, second, level, in_column, column_devices, send_2, recv_2)
    after_second[...] = value
    copies_3, value = stage(after_second, third, corner, in_plane, plane_devices, send_3, recv_3)
    total[...] = value
    for h in range(2):
        remote(tile, back.at[h], back_send.at[h], back_recv.at[h], back_devices[h]).wait_recv()
    times[...] = back[0] + back[1]
    for copy in returns + copies_1 + copies_2 + copies_3:
        copy.wait_send()


def reorder(tile, group, deltas):
    values = tile[0, : 2 * 2 * SEPS * PAIRS].reshape(2, 2, SEPS, PAIRS)
    mine = jnp.where(group == 0, values[0], values[1])
    picker = deltas[:, None] == jnp.arange(SEPS, dtype=jnp.int32)[None, :]
    return jnp.sum(jnp.where(picker[None, :, :, None], mine[:, None], 0.0), axis=2)


def per_device(fields, mom_pairs, deltas):
    group = lax.axis_index("mom")
    field = (2, 2, NEV, NEV)
    dma = pltpu.SemaphoreType.DMA
    tile = pl.pallas_call(
        trace_kernel,
        out_shape=jax.ShapeDtypeStruct((8, 128), jnp.float32),
        in_specs=[
            pl.BlockSpec(memory_space=pltpu.SMEM),
            pl.BlockSpec(memory_space=pltpu.VMEM),
            pl.BlockSpec(memory_space=pl.ANY),
        ],
        out_specs=pl.BlockSpec(memory_space=pltpu.VMEM),
        scratch_shapes=[
            pltpu.VMEM(field, jnp.bfloat16),
            pltpu.VMEM(field, jnp.bfloat16),
            pltpu.VMEM(field, jnp.bfloat16),
            pltpu.VMEM(field, jnp.bfloat16),
            pltpu.VMEM((2, *field), jnp.bfloat16),
            pltpu.VMEM((4, CHUNKS, 2 * ROWS, 2 * NEV), jnp.bfloat16),
            pltpu.VMEM((SEPS * PAIRS, NEV, NEV), jnp.float32),
            pltpu.VMEM((SEPS * PAIRS, NEV, NEV), jnp.float32),
            pltpu.VMEM((SEPS * PAIRS, 8, 128), jnp.float32),
            pltpu.VMEM((SEPS * PAIRS, 8, 128), jnp.float32),
            pltpu.VMEM((128, 128), jnp.float32),
            pltpu.VMEM((PAIRS, 2), jnp.int32),
            pltpu.SMEM((PAIRS, 2), jnp.int32),
            dma,
            dma((2,)),
            dma((2,)),
        ]
        + [dma((PIECES,))] * 8,
        compiler_params=pltpu.CompilerParams(
            collective_id=0, has_side_effects=True, vmem_limit_bytes=62 * 1024 * 1024
        ),
        name="traces",
    )(mom_pairs, mom_pairs, fields.reshape(field))
    times, total = pl.pallas_call(
        sum_kernel,
        out_shape=[jax.ShapeDtypeStruct((8, 128), jnp.float32)] * 2,
        in_specs=[pl.BlockSpec(memory_space=pltpu.VMEM)],
        out_specs=[pl.BlockSpec(memory_space=pltpu.VMEM)] * 2,
        scratch_shapes=[
            pltpu.VMEM((2, 8, 128), jnp.float32),
            pltpu.VMEM((8, 8, 128), jnp.float32),
            pltpu.VMEM((8, 8, 128), jnp.float32),
            pltpu.VMEM((4, 8, 128), jnp.float32),
            pltpu.VMEM((8, 128), jnp.float32),
            pltpu.VMEM((8, 128), jnp.float32),
            dma((2,)),
            dma((2,)),
            dma((7,)),
            dma((8,)),
            dma((7,)),
            dma((8,)),
            dma((3,)),
            dma((4,)),
        ],
        compiler_params=pltpu.CompilerParams(collective_id=1, has_side_effects=True),
        name="sums",
    )(tile)
    return reorder(times, group, deltas)[None], reorder(total, group, deltas)


def solution(mesh):
    return jax.shard_map(
        per_device,
        mesh=mesh,
        in_specs=(P("tm", "mom", None, None, None), P("mom", None), P()),
        out_specs=(P("tm", None, None, "mom"), P(None, None, "mom")),
        check_vma=False,
    )
```

```python
import functools

import jax
import jax.numpy as jnp
from jax import lax
from jax.experimental import pallas as pl
from jax.experimental.pallas import tpu as pltpu
from jax.sharding import PartitionSpec as P

MESH = pl.DeviceIdType.MESH
CHIPS_PER_PLANE = 32
ROWS = 128
CHUNKS = 4
SUB = 4
PIECES = CHUNKS * SUB
PIECE_ROWS = ROWS // SUB
NEV = ROWS * CHUNKS
PAIRS = 3
SEPS = 4


def place():
    time, group = lax.axis_index("tm"), lax.axis_index("mom")
    count = lax.axis_size("tm")
    chip, core = time // 2, time % 2
    swap_right = (chip % CHIPS_PER_PLANE) // (CHIPS_PER_PLANE - 1)
    swap_left = ((chip + 1) % CHIPS_PER_PLANE == 1).astype(jnp.int32)
    right = {"tm": (time + 2) % count, "mom": (group + swap_right) % 2}
    left = {"tm": (time + count - 2) % count, "mom": (group + swap_left) % 2}
    across = {"tm": time, "mom": 1 - group}
    partner = {"tm": time + 1 - 2 * core, "mom": group}
    return time, group, core, right, left, across, partner


def folded(values):
    total = values.reshape(-1, 8, values.shape[-1]).sum(0)
    lanes = [total[:, i : i + 128] for i in range(0, values.shape[-1], 128)]
    return functools.reduce(jnp.add, lanes)


def trace_kernel(
    pairs_own, pairs_sent, deltas, fields, tile,
    own, near, fed, ahead, source, wide, sums, flips, boxes, directs, rows_out, pairs_in, pairs_other,
    ready, load_sem, pair_sems, near_sems, send_right, recv_right, send_left, recv_left, send_y, recv_y, send_core, recv_core,
):
    time, group, core, right, left, across, partner = place()
    from_left = left["mom"]
    from_right = right["mom"]

    def rows(j):
        return pl.ds(pl.multiple_of(j * PIECE_ROWS, PIECE_ROWS), PIECE_ROWS)

    def remote(src, dst, send, recv, device):
        return pltpu.make_async_remote_copy(
            src_ref=src, dst_ref=dst, send_sem=send, recv_sem=recv, device_id=device, device_id_type=MESH
        )

    def to_right(j, held=own):
        return remote(
            held.at[:, :, rows(j), :], source.at[group, :, :, rows(j), :], send_right.at[j], recv_right.at[j], right
        )

    def to_left(j, held=own):
        return remote(held.at[:, :, rows(j), :], ahead.at[:, :, rows(j), :], send_left.at[j], recv_left.at[j], left)

    def over_y(j):
        part = source.at[from_left, :, :, rows(j), :]
        return remote(part, part, send_y.at[j], recv_y.at[j], across)

    def feed_source(j):
        return remote(
            source.at[from_left, :, :, rows(j), :], fed.at[:, :, rows(j), :], send_core.at[j], recv_core.at[j], partner
        )

    def feed_ahead(j):
        return remote(ahead.at[:, :, rows(j), :], fed.at[:, :, rows(j), :], send_core.at[j], recv_core.at[j], partner)

    near_copy = remote(fields, near, near_sems.at[0], near_sems.at[1], partner)
    pair_copy = remote(pairs_sent, pairs_in, pair_sems.at[0], pair_sems.at[1], across)
    load = pltpu.make_async_copy(fields, own, load_sem)

    barrier = pltpu.get_barrier_semaphore()
    for device in (left, across, partner):
        pl.semaphore_signal(barrier, inc=1, device_id=device, device_id_type=MESH)
    load.start()
    pl.semaphore_wait(barrier, 3)
    pl.semaphore_signal(ready, inc=1, device_id=right, device_id_type=MESH)

    @pl.when(core == 1)
    def _():
        @pl.loop(0, PIECES)
        def _(j):
            to_right(j, fields).start()

    @pl.when(core == 0)
    def _():
        pl.semaphore_wait(ready, 1)

        @pl.loop(0, PIECES)
        def _(j):
            to_left(j, fields).start()

    pair_copy.start()
    near_copy.start()

    @pl.loop(0, SEPS * PAIRS)
    def _(i):
        boxes[i] = jnp.zeros((8, 128), jnp.float32)
        directs[i] = jnp.zeros((8, 128), jnp.float32)

        @pl.loop(0, NEV // 32)
        def _(r):
            at = pl.ds(pl.multiple_of(r * 32, 32), 32)
            sums[i, at, :] = jnp.zeros((32, NEV), jnp.float32)
            flips[i, at, :] = jnp.zeros((32, NEV), jnp.float32)

    rows_out[...] = jnp.zeros_like(rows_out)
    load.wait()
    pair_copy.wait_recv()
    pair_load = pltpu.make_async_copy(pairs_in, pairs_other, load_sem)
    pair_load.start()
    pair_load.wait()

    @pl.when(core == 0)
    def _():
        @pl.loop(0, PIECES)
        def _(j):
            to_left(j).wait_recv()
            feed_ahead(j).start()

            @pl.when(j == PIECES - 3)
            def _():
                @pl.loop(0, PIECES)
                def _(k):
                    to_right(k).start()

    def pair(of_group, which, side):
        return jnp.where(of_group == group, pairs_own[side, which], pairs_other[side, which])

    def widen(n):
        at = pl.ds(pl.multiple_of(n * ROWS, ROWS), ROWS)
        for momentum in range(4):
            real = source[momentum // 2, momentum % 2, 0, at, :]
            imag = source[momentum // 2, momentum % 2, 1, at, :]
            wide[momentum, n, :ROWS, :NEV] = real
            wide[momentum, n, :ROWS, NEV:] = -imag
            wide[momentum, n, ROWS:, :NEV] = imag
            wide[momentum, n, ROWS:, NEV:] = real

    def work(slot, target, of_group, n):
        at = pl.ds(pl.multiple_of(n * ROWS, ROWS), ROWS)
        diagonal = (
            lax.broadcasted_iota(jnp.int32, (ROWS, NEV), 0) + n * ROWS
            == lax.broadcasted_iota(jnp.int32, (ROWS, NEV), 1)
        )
        for which in range(PAIRS):
            i = slot * PAIRS + which
            a = pair(of_group, which, 0)
            b = lax.rem(pair(of_group, which, 1), 2)
            full = jnp.dot(
                wide[a, n], target[b].reshape(2 * NEV, NEV), preferred_element_type=jnp.float32
            )
            real, imag = full[:ROWS], full[ROWS:]
            plus = real + imag
            flipped = (real - imag).T
            box = folded(plus * flips[i, at, :])
            sums[i, at, :] = plus
            flips[i, :, at] = flipped
            boxes[i] += box + folded(sums[i, :, at] * flipped)
            directs[i] += folded(jnp.where(diagonal, real, 0.0))

    fed_group = jnp.where(core == 0, from_left, from_right)
    fed_step = 2 + 3 * core
    ahead_step = 2 + (3 + CHUNKS) * core

    @pl.loop(0, 3 * CHUNKS + 1)
    def _(step):
        for q in range(SUB):

            @pl.when(step < CHUNKS)
            def _():
                j = step * SUB + q
                to_right(j).wait_recv()
                over_y(j).start()

                @pl.when(core == 1)
                def _():
                    feed_source(j).start()

            if q == 0:

                @pl.when(step == fed_step)
                def _():
                    @pl.loop(0, PIECES)
                    def _(j):
                        feed_ahead(j).wait_recv()

                @pl.when((step >= fed_step) & (step < fed_step + CHUNKS))
                def _():
                    work(2, fed, fed_group, step - fed_step)

            if q == 1:

                @pl.when((step == CHUNKS - 1) & (core == 1))
                def _():
                    pl.semaphore_wait(ready, 1)

                    @pl.loop(0, PIECES)
                    def _(j):
                        to_left(j).start()

                @pl.when((step == ahead_step) & (core == 1))
                def _():
                    @pl.loop(0, PIECES)
                    def _(j):
                        to_left(j).wait_recv()

                @pl.when((step >= ahead_step) & (step < ahead_step + CHUNKS))
                def _():
                    work(3, ahead, from_right, step - ahead_step)

            if q == 2:

                @pl.when((step >= 1) & (step <= CHUNKS))
                def _():
                    for piece in range(SUB):
                        over_y((step - 1) * SUB + piece).wait_recv()
                    widen(step - 1)
                    work(0, own, group, step - 1)

            if q == 3:

                @pl.when(step == 1)
                def _():
                    near_copy.wait_recv()

                @pl.when((step >= 1) & (step <= CHUNKS))
                def _():
                    work(1, near, group, step - 1)

    @pl.loop(0, PIECES)
    def _(j):
        to_right(j).wait_send()
        to_left(j).wait_send()
        over_y(j).wait_send()
        feed_ahead(j).wait_send()

    near_copy.wait_send()
    pair_copy.wait_send()

    separations = (1, 2 - 2 * core, 2 * core, 3)
    groups = (group, group, fed_group, from_right)
    lane = lax.broadcasted_iota(jnp.int32, (8, 128), 1)
    wanted = functools.reduce(
        jnp.add, [jnp.where(lane % SEPS == r, deltas[r], 0) for r in range(SEPS)]
    )
    for slot in range(SEPS):
        for kind, values in enumerate((directs, boxes)):
            for which in range(PAIRS):
                row = slot * 8 + which * 2 + kind
                rows_out[row : row + 1, :] = values[slot * PAIRS + which].sum(0, keepdims=True)
    totals = jnp.broadcast_to(rows_out[...].sum(1, keepdims=True), rows_out.shape)
    tile[...] = functools.reduce(
        jnp.add,
        [
            jnp.where(
                (wanted == separations[slot]) & (lane // SEPS == groups[slot]), totals[slot * 8 : slot * 8 + 8], 0.0
            )
            for slot in range(SEPS)
        ],
    )


def deliver(values, out, group):
    mine = jnp.where(group == 0, values[:, :SEPS], values[:, SEPS : 2 * SEPS])
    for which in range(PAIRS):
        out[which] = mine[which * 2 : which * 2 + 2]


def sum_kernel(
    tile, times, total, back, first, second, third, after_first, after_second,
    back_send, back_recv, send_1, recv_1, send_2, recv_2, send_3, recv_3,
):
    time, group = lax.axis_index("tm"), lax.axis_index("mom")
    count = lax.axis_size("tm")
    row, level, plane = time % 8, time // 8 % 8, time // 64
    before, behind = (time + count - 2) % count, (time + 2) % count
    in_row = [(row + d) % 8 for d in range(1, 8)]
    in_column = [(level + d) % 8 for d in range(1, 8)]
    corner = plane * 2 + group
    in_plane = [(corner + d) % 4 for d in range(1, 4)]
    row_devices = [{"tm": time - row + r, "mom": group} for r in in_row]
    column_devices = [{"tm": time + (r - level) * 8, "mom": group} for r in in_column]
    plane_devices = [{"tm": time + (r // 2 - plane) * 64, "mom": r % 2} for r in in_plane]
    back_devices = [{"tm": before, "mom": h} for h in range(2)]

    barrier = pltpu.get_barrier_semaphore()
    greeted = row_devices + column_devices + plane_devices + back_devices + [{"tm": behind, "mom": h} for h in range(2)]
    for device in greeted:
        pl.semaphore_signal(barrier, inc=1, device_id=device, device_id_type=MESH)
    pl.semaphore_wait(barrier, len(greeted))

    def remote(src, dst, send, recv, device):
        return pltpu.make_async_remote_copy(
            src_ref=src, dst_ref=dst, send_sem=send, recv_sem=recv, device_id=device, device_id_type=MESH
        )

    returns = [
        remote(tile, back.at[group], back_send.at[h], back_recv.at[group], device)
        for h, device in enumerate(back_devices)
    ]
    for copy in returns:
        copy.start()

    def stage(src, held, mine, places, devices, send, recv):
        copies = [
            remote(src, held.at[mine], send.at[d], recv.at[mine], device) for d, device in enumerate(devices)
        ]
        for copy in copies:
            copy.start()
        held[mine] = src[...]
        for d, place_of in enumerate(places):
            remote(src, held.at[place_of], send.at[d], recv.at[place_of], devices[d]).wait_recv()
        value = functools.reduce(jnp.add, [held[i] for i in range(held.shape[0])])
        return copies, value

    copies_1, value = stage(tile, first, row, in_row, row_devices, send_1, recv_1)
    after_first[...] = value
    copies_2, value = stage(after_first, second, level, in_column, column_devices, send_2, recv_2)
    after_second[...] = value
    copies_3, value = stage(after_second, third, corner, in_plane, plane_devices, send_3, recv_3)
    deliver(value, total, group)
    for h in range(2):
        remote(tile, back.at[h], back_send.at[h], back_recv.at[h], back_devices[h]).wait_recv()
    deliver(back[0] + back[1], times, group)
    for copy in returns + copies_1 + copies_2 + copies_3:
        copy.wait_send()


def per_device(fields, mom_pairs, deltas):
    field = (2, 2, NEV, NEV)
    dma = pltpu.SemaphoreType.DMA
    tile = pl.pallas_call(
        trace_kernel,
        out_shape=jax.ShapeDtypeStruct((8, 128), jnp.float32),
        in_specs=[
            pl.BlockSpec(memory_space=pltpu.SMEM),
            pl.BlockSpec(memory_space=pltpu.VMEM),
            pl.BlockSpec(memory_space=pltpu.SMEM),
            pl.BlockSpec(memory_space=pl.ANY),
        ],
        out_specs=pl.BlockSpec(memory_space=pltpu.VMEM),
        scratch_shapes=[
            pltpu.VMEM(field, jnp.bfloat16),
            pltpu.VMEM(field, jnp.bfloat16),
            pltpu.VMEM(field, jnp.bfloat16),
            pltpu.VMEM(field, jnp.bfloat16),
            pltpu.VMEM((2, *field), jnp.bfloat16),
            pltpu.VMEM((4, CHUNKS, 2 * ROWS, 2 * NEV), jnp.bfloat16),
            pltpu.VMEM((SEPS * PAIRS, NEV, NEV), jnp.float32),
            pltpu.VMEM((SEPS * PAIRS, NEV, NEV), jnp.float32),
            pltpu.VMEM((SEPS * PAIRS, 8, 128), jnp.float32),
            pltpu.VMEM((SEPS * PAIRS, 8, 128), jnp.float32),
            pltpu.VMEM((SEPS * 8, 128), jnp.float32),
            pltpu.VMEM((2, PAIRS), jnp.int32),
            pltpu.SMEM((2, PAIRS), jnp.int32),
            pltpu.SemaphoreType.REGULAR,
            dma,
            dma((2,)),
            dma((2,)),
        ]
        + [dma((PIECES,))] * 8,
        compiler_params=pltpu.CompilerParams(
            collective_id=0, has_side_effects=True, vmem_limit_bytes=62 * 1024 * 1024
        ),
        name="traces",
    )(mom_pairs.T, mom_pairs.T, deltas, fields.reshape(field))
    times, total = pl.pallas_call(
        sum_kernel,
        out_shape=[jax.ShapeDtypeStruct((PAIRS, 2, SEPS), jnp.float32)] * 2,
        in_specs=[pl.BlockSpec(memory_space=pltpu.VMEM)],
        out_specs=[pl.BlockSpec(memory_space=pltpu.VMEM)] * 2,
        scratch_shapes=[
            pltpu.VMEM((2, 8, 128), jnp.float32),
            pltpu.VMEM((8, 8, 128), jnp.float32),
            pltpu.VMEM((8, 8, 128), jnp.float32),
            pltpu.VMEM((4, 8, 128), jnp.float32),
            pltpu.VMEM((8, 128), jnp.float32),
            pltpu.VMEM((8, 128), jnp.float32),
            dma((2,)),
            dma((2,)),
            dma((7,)),
            dma((8,)),
            dma((7,)),
            dma((8,)),
            dma((3,)),
            dma((4,)),
        ],
        compiler_params=pltpu.CompilerParams(collective_id=1, has_side_effects=True),
        name="sums",
    )(tile)
    return times.transpose(1, 2, 0)[None], total.transpose(1, 2, 0)


def solution(mesh):
    return jax.shard_map(
        per_device,
        mesh=mesh,
        in_specs=(P("tm", "mom", None, None, None), P("mom", None), P()),
        out_specs=(P("tm", None, None, "mom"), P(None, None, "mom")),
        check_vma=False,
    )
```

```python
import functools

import jax
import jax.numpy as jnp
from jax import lax
from jax.experimental import pallas as pl
from jax.experimental.pallas import tpu as pltpu
from jax.sharding import PartitionSpec as P

MESH = pl.DeviceIdType.MESH
CHIPS_PER_PLANE = 32
ROWS = 128
CHUNKS = 4
SUB = 4
PIECES = CHUNKS * SUB
PIECE_ROWS = ROWS // SUB
NEV = ROWS * CHUNKS
PAIRS = 3
SEPS = 4


def place():
    time, group = lax.axis_index("tm"), lax.axis_index("mom")
    count = lax.axis_size("tm")
    chip, core = time // 2, time % 2
    swap_right = (chip % CHIPS_PER_PLANE) // (CHIPS_PER_PLANE - 1)
    swap_left = ((chip + 1) % CHIPS_PER_PLANE == 1).astype(jnp.int32)
    right = {"tm": (time + 2) % count, "mom": (group + swap_right) % 2}
    left = {"tm": (time + count - 2) % count, "mom": (group + swap_left) % 2}
    across = {"tm": time, "mom": 1 - group}
    partner = {"tm": time + 1 - 2 * core, "mom": group}
    return time, group, core, right, left, across, partner


def folded(values):
    total = values.reshape(-1, 8, values.shape[-1]).sum(0)
    lanes = [total[:, i : i + 128] for i in range(0, values.shape[-1], 128)]
    return functools.reduce(jnp.add, lanes)


def trace_kernel(
    pairs_own, pairs_sent, deltas, fields, results,
    own, near, fed, ahead, source, wide, sums, flips, boxes, directs, rows_out, pairs_in, pairs_other,
    tile, back, first, second, third, after_first, after_second, load_sem, pair_sems, near_sems, send_right, recv_right, send_left, recv_left, send_y, recv_y, send_core, recv_core,
    back_send, back_recv, send_1, recv_1, send_2, recv_2, send_3, recv_3,
):
    time, group, core, right, left, across, partner = place()
    from_left = left["mom"]
    from_right = right["mom"]

    def rows(j):
        return pl.ds(pl.multiple_of(j * PIECE_ROWS, PIECE_ROWS), PIECE_ROWS)

    def remote(src, dst, send, recv, device):
        return pltpu.make_async_remote_copy(
            src_ref=src, dst_ref=dst, send_sem=send, recv_sem=recv, device_id=device, device_id_type=MESH
        )

    def to_right(j, held=own):
        return remote(
            held.at[:, :, rows(j), :], source.at[group, :, :, rows(j), :], send_right.at[j], recv_right.at[j], right
        )

    def to_left(j, held=own):
        return remote(held.at[:, :, rows(j), :], ahead.at[:, :, rows(j), :], send_left.at[j], recv_left.at[j], left)

    def over_y(j):
        part = source.at[from_left, :, :, rows(j), :]
        return remote(part, part, send_y.at[j], recv_y.at[j], across)

    def feed_source(j):
        return remote(
            source.at[from_left, :, :, rows(j), :], fed.at[:, :, rows(j), :], send_core.at[j], recv_core.at[j], partner
        )

    def feed_ahead(j):
        return remote(ahead.at[:, :, rows(j), :], fed.at[:, :, rows(j), :], send_core.at[j], recv_core.at[j], partner)

    near_copy = remote(fields, near, near_sems.at[0], near_sems.at[1], partner)
    pair_copy = remote(pairs_sent, pairs_in, pair_sems.at[0], pair_sems.at[1], across)
    load = pltpu.make_async_copy(fields, own, load_sem)

    count = lax.axis_size("tm")
    row, level, plane = time % 8, time // 8 % 8, time // 64
    in_row = [(row + d) % 8 for d in range(1, 8)]
    in_column = [(level + d) % 8 for d in range(1, 8)]
    corner = plane * 2 + group
    in_plane = [(corner + d) % 4 for d in range(1, 4)]
    row_devices = [{"tm": time - row + r, "mom": group} for r in in_row]
    column_devices = [{"tm": time + (r - level) * 8, "mom": group} for r in in_column]
    plane_devices = [{"tm": time + (r // 2 - plane) * 64, "mom": r % 2} for r in in_plane]
    back_devices = [{"tm": (time + count - 2) % count, "mom": h} for h in range(2)]
    behind_devices = [{"tm": (time + 2) % count, "mom": h} for h in range(2)]

    barrier = pltpu.get_barrier_semaphore()
    greeted = column_devices + plane_devices + row_devices + back_devices + behind_devices
    for device in greeted:
        pl.semaphore_signal(barrier, inc=1, device_id=device, device_id_type=MESH)
    load.start()
    pl.semaphore_wait(barrier, len(greeted))

    @pl.when(core == 1)
    def _():
        @pl.loop(0, PIECES)
        def _(j):
            to_right(j, fields).start()

    @pl.when(core == 0)
    def _():
        @pl.loop(0, PIECES)
        def _(j):
            to_left(j, fields).start()

    pair_copy.start()
    near_copy.start()

    @pl.loop(0, SEPS * PAIRS)
    def _(i):
        boxes[i] = jnp.zeros((8, 128), jnp.float32)
        directs[i] = jnp.zeros((8, 128), jnp.float32)

        @pl.loop(0, NEV // 32)
        def _(r):
            at = pl.ds(pl.multiple_of(r * 32, 32), 32)
            sums[i, at, :] = jnp.zeros((32, NEV), jnp.float32)
            flips[i, at, :] = jnp.zeros((32, NEV), jnp.float32)

    rows_out[...] = jnp.zeros_like(rows_out)
    load.wait()
    pair_copy.wait_recv()
    pair_load = pltpu.make_async_copy(pairs_in, pairs_other, load_sem)
    pair_load.start()
    pair_load.wait()

    @pl.when(core == 0)
    def _():
        @pl.loop(0, PIECES)
        def _(j):
            to_left(j).wait_recv()
            feed_ahead(j).start()

            @pl.when(j == PIECES - 3)
            def _():
                @pl.loop(0, PIECES)
                def _(k):
                    to_right(k).start()

    def pair(of_group, which, side):
        return jnp.where(of_group == group, pairs_own[side, which], pairs_other[side, which])

    def widen(n):
        at = pl.ds(pl.multiple_of(n * ROWS, ROWS), ROWS)
        for momentum in range(4):
            real = source[momentum // 2, momentum % 2, 0, at, :]
            imag = source[momentum // 2, momentum % 2, 1, at, :]
            wide[momentum, n, :ROWS, :NEV] = real
            wide[momentum, n, :ROWS, NEV:] = -imag
            wide[momentum, n, ROWS:, :NEV] = imag
            wide[momentum, n, ROWS:, NEV:] = real

    def work(slot, target, of_group, n):
        at = pl.ds(pl.multiple_of(n * ROWS, ROWS), ROWS)
        diagonal = (
            lax.broadcasted_iota(jnp.int32, (ROWS, NEV), 0) + n * ROWS
            == lax.broadcasted_iota(jnp.int32, (ROWS, NEV), 1)
        )
        for which in range(PAIRS):
            i = slot * PAIRS + which
            a = pair(of_group, which, 0)
            b = lax.rem(pair(of_group, which, 1), 2)
            full = jnp.dot(
                wide[a, n], target[b].reshape(2 * NEV, NEV), preferred_element_type=jnp.float32
            )
            real, imag = full[:ROWS], full[ROWS:]
            plus = real + imag
            flipped = (real - imag).T
            box = folded(plus * flips[i, at, :])
            sums[i, at, :] = plus
            flips[i, :, at] = flipped
            boxes[i] += box + folded(sums[i, :, at] * flipped)
            directs[i] += folded(jnp.where(diagonal, real, 0.0))

    fed_group = jnp.where(core == 0, from_left, from_right)
    fed_step = 2 + 3 * core
    ahead_step = 2 + (3 + CHUNKS) * core

    @pl.loop(0, 3 * CHUNKS + 1)
    def _(step):
        for q in range(SUB):

            @pl.when(step < CHUNKS)
            def _():
                j = step * SUB + q
                to_right(j).wait_recv()
                over_y(j).start()

                @pl.when(core == 1)
                def _():
                    feed_source(j).start()

            if q == 0:

                @pl.when(step == fed_step)
                def _():
                    @pl.loop(0, PIECES)
                    def _(j):
                        feed_ahead(j).wait_recv()

                @pl.when((step >= fed_step) & (step < fed_step + CHUNKS))
                def _():
                    work(2, fed, fed_group, step - fed_step)

            if q == 1:

                @pl.when((step == ahead_step) & (core == 1))
                def _():
                    @pl.loop(0, PIECES)
                    def _(j):
                        to_left(j).wait_recv()

                @pl.when((step >= ahead_step) & (step < ahead_step + CHUNKS))
                def _():
                    work(3, ahead, from_right, step - ahead_step)

            if q == 2:

                @pl.when((step == CHUNKS - 1) & (core == 1))
                def _():
                    @pl.loop(0, PIECES)
                    def _(j):
                        to_left(j).start()

                @pl.when((step >= 1) & (step <= CHUNKS))
                def _():
                    for piece in range(SUB):
                        over_y((step - 1) * SUB + piece).wait_recv()
                    widen(step - 1)
                    work(0, own, group, step - 1)

            if q == 3:

                @pl.when(step == 1)
                def _():
                    near_copy.wait_recv()

                @pl.when((step >= 1) & (step <= CHUNKS))
                def _():
                    work(1, near, group, step - 1)

    separations = (1, 2 - 2 * core, 2 * core, 3)
    groups = (group, group, fed_group, from_right)
    lane = lax.broadcasted_iota(jnp.int32, (8, 128), 1)
    wanted = functools.reduce(
        jnp.add, [jnp.where(lane % SEPS == r, deltas[r], 0) for r in range(SEPS)]
    )
    for slot in range(SEPS):
        for kind, values in enumerate((directs, boxes)):
            for which in range(PAIRS):
                line = slot * 8 + which * 2 + kind
                rows_out[line : line + 1, :] = values[slot * PAIRS + which].sum(0, keepdims=True)
    totals = jnp.broadcast_to(rows_out[...].sum(1, keepdims=True), rows_out.shape)
    tile[...] = functools.reduce(
        jnp.add,
        [
            jnp.where(
                (wanted == separations[slot]) & (lane // SEPS == groups[slot]), totals[slot * 8 : slot * 8 + 8], 0.0
            )
            for slot in range(SEPS)
        ],
    )

    returns = [
        remote(tile, back.at[group], back_send.at[h], back_recv.at[group], device)
        for h, device in enumerate(back_devices)
    ]
    for copy in returns:
        copy.start()

    def stage(src, held, mine, places, devices, send, recv):
        copies = [
            remote(src, held.at[mine], send.at[d], recv.at[mine], device) for d, device in enumerate(devices)
        ]
        for copy in copies:
            copy.start()
        held[mine] = src[...]
        for d, place_of in enumerate(places):
            remote(src, held.at[place_of], send.at[d], recv.at[place_of], devices[d]).wait_recv()
        return copies, functools.reduce(jnp.add, [held[i] for i in range(held.shape[0])])

    def deliver(values, out):
        mine = jnp.where(group == 0, values[:, :SEPS], values[:, SEPS : 2 * SEPS])
        for which in range(PAIRS):
            results[out, which] = mine[which * 2 : which * 2 + 2]

    copies_1, value = stage(tile, first, row, in_row, row_devices, send_1, recv_1)
    after_first[...] = value
    copies_2, value = stage(after_first, second, level, in_column, column_devices, send_2, recv_2)
    after_second[...] = value
    copies_3, value = stage(after_second, third, corner, in_plane, plane_devices, send_3, recv_3)
    deliver(value, 1)
    for h in range(2):
        remote(tile, back.at[h], back_send.at[h], back_recv.at[h], back_devices[h]).wait_recv()
    deliver(back[0] + back[1], 0)
    for copy in returns + copies_1 + copies_2 + copies_3:
        copy.wait_send()

    @pl.loop(0, PIECES)
    def _(j):
        to_right(j).wait_send()
        to_left(j).wait_send()
        over_y(j).wait_send()
        feed_ahead(j).wait_send()

    near_copy.wait_send()
    pair_copy.wait_send()


def per_device(fields, mom_pairs, deltas):
    field = (2, 2, NEV, NEV)
    dma = pltpu.SemaphoreType.DMA
    results = pl.pallas_call(
        trace_kernel,
        out_shape=jax.ShapeDtypeStruct((2, PAIRS, 2, SEPS), jnp.float32),
        in_specs=[
            pl.BlockSpec(memory_space=pltpu.SMEM),
            pl.BlockSpec(memory_space=pltpu.VMEM),
            pl.BlockSpec(memory_space=pltpu.SMEM),
            pl.BlockSpec(memory_space=pl.ANY),
        ],
        out_specs=pl.BlockSpec(memory_space=pltpu.VMEM),
        scratch_shapes=[
            pltpu.VMEM(field, jnp.bfloat16),
            pltpu.VMEM(field, jnp.bfloat16),
            pltpu.VMEM(field, jnp.bfloat16),
            pltpu.VMEM(field, jnp.bfloat16),
            pltpu.VMEM((2, *field), jnp.bfloat16),
            pltpu.VMEM((4, CHUNKS, 2 * ROWS, 2 * NEV), jnp.bfloat16),
            pltpu.VMEM((SEPS * PAIRS, NEV, NEV), jnp.float32),
            pltpu.VMEM((SEPS * PAIRS, NEV, NEV), jnp.float32),
            pltpu.VMEM((SEPS * PAIRS, 8, 128), jnp.float32),
            pltpu.VMEM((SEPS * PAIRS, 8, 128), jnp.float32),
            pltpu.VMEM((SEPS * 8, 128), jnp.float32),
            pltpu.VMEM((2, PAIRS), jnp.int32),
            pltpu.SMEM((2, PAIRS), jnp.int32),
            pltpu.VMEM((8, 128), jnp.float32),
            pltpu.VMEM((2, 8, 128), jnp.float32),
            pltpu.VMEM((8, 8, 128), jnp.float32),
            pltpu.VMEM((8, 8, 128), jnp.float32),
            pltpu.VMEM((4, 8, 128), jnp.float32),
            pltpu.VMEM((8, 128), jnp.float32),
            pltpu.VMEM((8, 128), jnp.float32),
            dma,
            dma((2,)),
            dma((2,)),
        ]
        + [dma((PIECES,))] * 8
        + [dma((n,)) for n in (2, 2, 7, 8, 7, 8, 3, 4)],
        compiler_params=pltpu.CompilerParams(
            collective_id=0, has_side_effects=True, vmem_limit_bytes=62 * 1024 * 1024
        ),
        name="traces",
    )(mom_pairs.T, mom_pairs.T, deltas, fields.reshape(field))
    times, total = results.transpose(0, 2, 3, 1)
    return times[None], total


def solution(mesh):
    return jax.shard_map(
        per_device,
        mesh=mesh,
        in_specs=(P("tm", "mom", None, None, None), P("mom", None), P()),
        out_specs=(P("tm", None, None, "mom"), P(None, None, "mom")),
        check_vma=False,
    )
```

```python
import functools

import jax
import jax.numpy as jnp
from jax import lax
from jax.experimental import pallas as pl
from jax.experimental.pallas import tpu as pltpu
from jax.sharding import PartitionSpec as P

MESH = pl.DeviceIdType.MESH
CHIPS_PER_PLANE = 32
ROWS = 128
CHUNKS = 4
SUB = 4
PIECES = CHUNKS * SUB
PIECE_ROWS = ROWS // SUB
NEV = ROWS * CHUNKS
PAIRS = 3
SEPS = 4


def place():
    time, group = lax.axis_index("tm"), lax.axis_index("mom")
    count = lax.axis_size("tm")
    chip, core = time // 2, time % 2
    swap_right = (chip % CHIPS_PER_PLANE) // (CHIPS_PER_PLANE - 1)
    swap_left = ((chip + 1) % CHIPS_PER_PLANE == 1).astype(jnp.int32)
    right = {"tm": (time + 2) % count, "mom": (group + swap_right) % 2}
    left = {"tm": (time + count - 2) % count, "mom": (group + swap_left) % 2}
    across = {"tm": time, "mom": 1 - group}
    partner = {"tm": time + 1 - 2 * core, "mom": group}
    return time, group, core, right, left, across, partner


def folded(values):
    total = values.reshape(-1, 8, values.shape[-1]).sum(0)
    lanes = [total[:, i : i + 128] for i in range(0, values.shape[-1], 128)]
    return functools.reduce(jnp.add, lanes)


def trace_kernel(
    pairs, deltas_in, fields, results,
    own, near, fed, ahead, relay, source, wide, sums, flips, boxes, directs, rows_out, pairs_in, pairs_own, pairs_other, deltas,
    tile, back, first, second, third, after_first, after_second, load_sem, pair_sems, near_sems, send_right, recv_right, send_left, recv_left, send_y, recv_y, send_core, recv_core,
    recv_relay, relay_sent_y, relay_sent_core,
    back_send, back_recv, send_1, recv_1, send_2, recv_2, send_3, recv_3,
):
    time, group, core, right, left, across, partner = place()
    count = lax.axis_size("tm")
    from_left = left["mom"]
    from_right = right["mom"]

    def rows(j):
        return pl.ds(pl.multiple_of(j * PIECE_ROWS, PIECE_ROWS), PIECE_ROWS)

    def remote(src, dst, send, recv, device):
        return pltpu.make_async_remote_copy(
            src_ref=src, dst_ref=dst, send_sem=send, recv_sem=recv, device_id=device, device_id_type=MESH
        )

    def to_right(j, held=own):
        return remote(
            held.at[:, :, rows(j), :], source.at[group, :, :, rows(j), :], send_right.at[j], recv_right.at[j], right
        )

    def to_left(j, held=own):
        return remote(held.at[:, :, rows(j), :], ahead.at[:, :, rows(j), :], send_left.at[j], recv_left.at[j], left)

    def to_relay(j):
        device = {"tm": (time + 3) % count, "mom": right["mom"]}
        return remote(
            own.at[:, :, rows(j), :], relay.at[:, :, rows(j), :], send_right.at[j], recv_relay.at[j], device
        )

    def relay_y(j):
        part = source.at[from_left, :, :, rows(j), :]
        device = {"tm": partner["tm"], "mom": 1 - group}
        return remote(relay.at[:, :, rows(j), :], part, relay_sent_y.at[j], recv_y.at[j], device)

    def relay_core(j):
        part = source.at[from_left, :, :, rows(j), :]
        return remote(relay.at[:, :, rows(j), :], part, relay_sent_core.at[j], recv_right.at[j], partner)

    def over_y(j):
        part = source.at[from_left, :, :, rows(j), :]
        return remote(part, part, send_y.at[j], recv_y.at[j], across)

    def feed_source(j):
        return remote(
            source.at[from_left, :, :, rows(j), :], fed.at[:, :, rows(j), :], send_core.at[j], recv_core.at[j], partner
        )

    def feed_ahead(j):
        return remote(ahead.at[:, :, rows(j), :], fed.at[:, :, rows(j), :], send_core.at[j], recv_core.at[j], partner)

    near_copy = remote(fields, near, near_sems.at[0], near_sems.at[1], partner)
    pair_copy = remote(pairs, pairs_in, pair_sems.at[0], pair_sems.at[1], across)
    load = pltpu.make_async_copy(fields, own, load_sem)

    row, level, plane = time % 8, time // 8 % 8, time // 64
    in_row = [(row + d) % 8 for d in range(1, 8)]
    in_column = [(level + d) % 8 for d in range(1, 8)]
    corner = plane * 2 + group
    in_plane = [(corner + d) % 4 for d in range(1, 4)]
    row_devices = [{"tm": time - row + r, "mom": group} for r in in_row]
    column_devices = [{"tm": time + (r - level) * 8, "mom": group} for r in in_column]
    plane_devices = [{"tm": time + (r // 2 - plane) * 64, "mom": r % 2} for r in in_plane]
    back_devices = [{"tm": (time + count - 2) % count, "mom": h} for h in range(2)]
    behind_devices = [{"tm": (time + 2) % count, "mom": h} for h in range(2)]

    barrier = pltpu.get_barrier_semaphore()
    relays = [
        {"tm": partner["tm"], "mom": 1 - group},
        {"tm": (time + count + 3 - 6 * core) % count, "mom": jnp.where(core == 0, right["mom"], left["mom"])},
    ]
    greeted = column_devices + plane_devices + row_devices + back_devices + behind_devices + relays
    for device in greeted:
        pl.semaphore_signal(barrier, inc=1, device_id=device, device_id_type=MESH)
    own_tables = [
        pltpu.make_async_copy(pairs, pairs_own, pair_sems.at[2]),
        pltpu.make_async_copy(deltas_in, deltas, pair_sems.at[3]),
    ]
    load.start()
    for copy in own_tables:
        copy.start()
    pl.semaphore_wait(barrier, len(greeted))

    @pl.when(core == 1)
    def _():
        @pl.loop(0, PIECES)
        def _(j):
            to_right(j, fields).start()

    @pl.when(core == 0)
    def _():
        @pl.loop(0, PIECES)
        def _(j):
            to_left(j, fields).start()

    pair_copy.start()
    near_copy.start()

    @pl.loop(0, SEPS * PAIRS)
    def _(i):
        boxes[i] = jnp.zeros((8, 128), jnp.float32)
        directs[i] = jnp.zeros((8, 128), jnp.float32)

        @pl.loop(0, NEV // 32)
        def _(r):
            at = pl.ds(pl.multiple_of(r * 32, 32), 32)
            sums[i, at, :] = jnp.zeros((32, NEV), jnp.float32)
            flips[i, at, :] = jnp.zeros((32, NEV), jnp.float32)

    rows_out[...] = jnp.zeros_like(rows_out)
    load.wait()
    for copy in own_tables:
        copy.wait()
    pair_copy.wait_recv()
    pair_load = pltpu.make_async_copy(pairs_in, pairs_other, load_sem)
    pair_load.start()
    pair_load.wait()

    def pair(of_group, which, side):
        return jnp.where(of_group == group, pairs_own[side, which], pairs_other[side, which])

    def widen(n):
        at = pl.ds(pl.multiple_of(n * ROWS, ROWS), ROWS)
        for momentum in range(4):
            real = source[momentum // 2, momentum % 2, 0, at, :]
            imag = source[momentum // 2, momentum % 2, 1, at, :]
            wide[momentum, n, :ROWS, :NEV] = real
            wide[momentum, n, :ROWS, NEV:] = -imag
            wide[momentum, n, ROWS:, :NEV] = imag
            wide[momentum, n, ROWS:, NEV:] = real

    def work(targets, n):
        at = pl.ds(pl.multiple_of(n * ROWS, ROWS), ROWS)
        diagonal = (
            lax.broadcasted_iota(jnp.int32, (ROWS, NEV), 0) + n * ROWS
            == lax.broadcasted_iota(jnp.int32, (ROWS, NEV), 1)
        )
        for slot, target, of_group in targets:
            for which in range(PAIRS):
                i = slot * PAIRS + which
                a = pair(of_group, which, 0)
                b = lax.rem(pair(of_group, which, 1), 2)
                full = jnp.dot(
                    wide[a, n], target[b].reshape(2 * NEV, NEV), preferred_element_type=jnp.float32
                )
                real, imag = full[:ROWS], full[ROWS:]
                plus = real + imag
                flipped = (real - imag).T
                box = folded(plus * flips[i, at, :])
                sums[i, at, :] = plus
                flips[i, :, at] = flipped
                boxes[i] += box + folded(sums[i, :, at] * flipped)
                directs[i] += folded(jnp.where(diagonal, real, 0.0))

    fed_group = jnp.where(core == 0, from_left, from_right)
    own_part, near_part = (0, own, group), (1, near, group)
    fed_part, ahead_part = (2, fed, fed_group), (3, ahead, from_right)
    nearly = PIECES - 2

    @pl.when(core == 0)
    def _():
        @pl.loop(0, nearly)
        def _(j):
            to_left(j).wait_send()

        @pl.loop(0, PIECES)
        def _(j):
            to_relay(j).start()

        @pl.loop(0, PIECES)
        def _(j):
            to_left(j).wait_recv()
            feed_ahead(j).start()

        @pl.loop(0, PIECES)
        def _(j):
            feed_source(j).wait_recv()

        near_copy.wait_recv()

        @pl.loop(0, CHUNKS)
        def _(n):
            for q in range(SUB):
                relay_core(n * SUB + q).wait_recv()
                relay_y(n * SUB + q).wait_recv()
            widen(n)
            work([own_part, near_part, fed_part, ahead_part], n)

    @pl.when(core == 1)
    def _():
        @pl.loop(0, 2 * CHUNKS)
        def _(step):
            for q in range(SUB):

                @pl.when(step < CHUNKS)
                def _():
                    j = step * SUB + q
                    to_right(j).wait_recv()
                    over_y(j).start()
                    feed_source(j).start()

                @pl.when(step >= CHUNKS)
                def _():
                    j = (step - CHUNKS) * SUB + q
                    to_relay(j).wait_recv()
                    relay_y(j).start()
                    relay_core(j).start()

                if q == 1:

                    @pl.when(step == CHUNKS - 1)
                    def _():
                        @pl.loop(0, nearly)
                        def _(j):
                            to_right(j).wait_send()

                        @pl.loop(0, PIECES)
                        def _(j):
                            to_left(j).start()

                if q == 2:

                    @pl.when(step == 1)
                    def _():
                        near_copy.wait_recv()

                    @pl.when((step >= 1) & (step <= CHUNKS))
                    def _():
                        for piece in range(SUB):
                            over_y((step - 1) * SUB + piece).wait_recv()
                        widen(step - 1)
                        work([own_part, near_part], step - 1)

                if q == 0:

                    @pl.when(step == CHUNKS + 1)
                    def _():
                        @pl.loop(0, PIECES)
                        def _(j):
                            feed_ahead(j).wait_recv()

                        @pl.loop(0, CHUNKS // 2)
                        def _(n):
                            work([fed_part], n)

                    @pl.when(step == CHUNKS + 2)
                    def _():
                        @pl.loop(CHUNKS // 2, CHUNKS)
                        def _(n):
                            work([fed_part], n)

        @pl.loop(0, PIECES)
        def _(j):
            to_left(j).wait_recv()

        @pl.loop(0, CHUNKS)
        def _(n):
            work([ahead_part], n)

    separations = (1, 2 - 2 * core, 2 * core, 3)
    groups = (group, group, fed_group, from_right)
    lane = lax.broadcasted_iota(jnp.int32, (8, 128), 1)
    wanted = functools.reduce(
        jnp.add, [jnp.where(lane % SEPS == r, deltas[r], 0) for r in range(SEPS)]
    )
    for slot in range(SEPS):
        for kind, values in enumerate((directs, boxes)):
            for which in range(PAIRS):
                line = slot * 8 + which * 2 + kind
                rows_out[line : line + 1, :] = values[slot * PAIRS + which].sum(0, keepdims=True)
    totals = jnp.broadcast_to(rows_out[...].sum(1, keepdims=True), rows_out.shape)
    tile[...] = functools.reduce(
        jnp.add,
        [
            jnp.where(
                (wanted == separations[slot]) & (lane // SEPS == groups[slot]), totals[slot * 8 : slot * 8 + 8], 0.0
            )
            for slot in range(SEPS)
        ],
    )

    returns = [
        remote(tile, back.at[group], back_send.at[h], back_recv.at[group], device)
        for h, device in enumerate(back_devices)
    ]
    for copy in returns:
        copy.start()

    def sent():
        @pl.when(core == 0)
        def _():
            @pl.loop(nearly, PIECES)
            def _(j):
                to_left(j).wait_send()

            @pl.loop(0, PIECES)
            def _(j):
                to_relay(j).wait_send()
                feed_ahead(j).wait_send()

        @pl.when(core == 1)
        def _():
            @pl.loop(nearly, PIECES)
            def _(j):
                to_right(j).wait_send()

            @pl.loop(0, PIECES)
            def _(j):
                to_left(j).wait_send()
                over_y(j).wait_send()
                feed_source(j).wait_send()
                relay_y(j).wait_send()
                relay_core(j).wait_send()

        near_copy.wait_send()
        pair_copy.wait_send()

    def stage(src, held, mine, places, devices, send, recv):
        copies = [
            remote(src, held.at[mine], send.at[d], recv.at[mine], device) for d, device in enumerate(devices)
        ]
        for copy in copies:
            copy.start()
        held[mine] = src[...]
        if held is first:
            sent()
        for d, place_of in enumerate(places):
            remote(src, held.at[place_of], send.at[d], recv.at[place_of], devices[d]).wait_recv()
        return copies, functools.reduce(jnp.add, [held[i] for i in range(held.shape[0])])

    def deliver(values, out):
        mine = jnp.where(group == 0, values[:, :SEPS], values[:, SEPS : 2 * SEPS])
        for which in range(PAIRS):
            results[out, which] = mine[which * 2 : which * 2 + 2]

    copies_1, value = stage(tile, first, row, in_row, row_devices, send_1, recv_1)
    after_first[...] = value
    copies_2, value = stage(after_first, second, level, in_column, column_devices, send_2, recv_2)
    after_second[...] = value
    copies_3, value = stage(after_second, third, corner, in_plane, plane_devices, send_3, recv_3)
    deliver(value, 1)
    for h in range(2):
        remote(tile, back.at[h], back_send.at[h], back_recv.at[h], back_devices[h]).wait_recv()
    deliver(back[0] + back[1], 0)
    for copy in returns + copies_1 + copies_2 + copies_3:
        copy.wait_send()


def per_device(fields, mom_pairs, deltas):
    field = (2, 2, NEV, NEV)
    dma = pltpu.SemaphoreType.DMA
    results = pl.pallas_call(
        trace_kernel,
        out_shape=jax.ShapeDtypeStruct((2, PAIRS, 2, SEPS), jnp.float32),
        in_specs=[
            pl.BlockSpec(memory_space=pl.ANY),
            pl.BlockSpec(memory_space=pl.ANY),
            pl.BlockSpec(memory_space=pl.ANY),
        ],
        out_specs=pl.BlockSpec(memory_space=pltpu.VMEM),
        scratch_shapes=[
            pltpu.VMEM(field, jnp.bfloat16),
            pltpu.VMEM(field, jnp.bfloat16),
            pltpu.VMEM(field, jnp.bfloat16),
            pltpu.VMEM(field, jnp.bfloat16),
            pltpu.VMEM(field, jnp.bfloat16),
            pltpu.VMEM((2, *field), jnp.bfloat16),
            pltpu.VMEM((4, CHUNKS, 2 * ROWS, 2 * NEV), jnp.bfloat16),
            pltpu.VMEM((SEPS * PAIRS, NEV, NEV), jnp.float32),
            pltpu.VMEM((SEPS * PAIRS, NEV, NEV), jnp.float32),
            pltpu.VMEM((SEPS * PAIRS, 8, 128), jnp.float32),
            pltpu.VMEM((SEPS * PAIRS, 8, 128), jnp.float32),
            pltpu.VMEM((SEPS * 8, 128), jnp.float32),
            pltpu.VMEM((2, PAIRS), jnp.int32),
            pltpu.SMEM((2, PAIRS), jnp.int32),
            pltpu.SMEM((2, PAIRS), jnp.int32),
            pltpu.SMEM((SEPS,), jnp.int32),
            pltpu.VMEM((8, 128), jnp.float32),
            pltpu.VMEM((2, 8, 128), jnp.float32),
            pltpu.VMEM((8, 8, 128), jnp.float32),
            pltpu.VMEM((8, 8, 128), jnp.float32),
            pltpu.VMEM((4, 8, 128), jnp.float32),
            pltpu.VMEM((8, 128), jnp.float32),
            pltpu.VMEM((8, 128), jnp.float32),
            dma,
            dma((4,)),
            dma((2,)),
        ]
        + [dma((PIECES,))] * 11
        + [dma((n,)) for n in (2, 2, 7, 8, 7, 8, 3, 4)],
        compiler_params=pltpu.CompilerParams(
            collective_id=0, has_side_effects=True, vmem_limit_bytes=62 * 1024 * 1024
        ),
        name="traces",
    )(mom_pairs.T, deltas, fields.reshape(field))
    times, total = results.transpose(0, 2, 3, 1)
    return times[None], total


def solution(mesh):
    return jax.shard_map(
        per_device,
        mesh=mesh,
        in_specs=(P("tm", "mom", None, None, None), P("mom", None), P()),
        out_specs=(P("tm", None, None, "mom"), P(None, None, "mom")),
        check_vma=False,
    )
```

```python
import functools

import jax
import jax.numpy as jnp
from jax import lax
from jax.experimental import pallas as pl
from jax.experimental.pallas import tpu as pltpu
from jax.sharding import PartitionSpec as P

MESH = pl.DeviceIdType.MESH
CHIPS_PER_PLANE = 32
ROWS = 128
CHUNKS = 4
LEVELS, LEVEL_DEVICES = 8, 32
SUB = 4
PIECES = CHUNKS * SUB
PIECE_ROWS = ROWS // SUB
NEV = ROWS * CHUNKS
PAIRS = 3
SEPS = 4


def place():
    time, group = lax.axis_index("tm"), lax.axis_index("mom")
    count = lax.axis_size("tm")
    chip, core = time // 2, time % 2
    swap_right = (chip % CHIPS_PER_PLANE) // (CHIPS_PER_PLANE - 1)
    swap_left = ((chip + 1) % CHIPS_PER_PLANE == 1).astype(jnp.int32)
    right = {"tm": (time + 2) % count, "mom": (group + swap_right) % 2}
    left = {"tm": (time + count - 2) % count, "mom": (group + swap_left) % 2}
    across = {"tm": time, "mom": 1 - group}
    partner = {"tm": time + 1 - 2 * core, "mom": group}
    return time, group, core, right, left, across, partner


def folded(values):
    total = values.reshape(-1, 8, values.shape[-1]).sum(0)
    lanes = [total[:, i : i + 128] for i in range(0, values.shape[-1], 128)]
    return functools.reduce(jnp.add, lanes)


def trace_kernel(
    pairs, deltas_in, fields, results,
    own, near, fed, ahead, relay, source, wide, sums, flips, boxes, directs, rows_out, pairs_in, pairs_own, pairs_other, deltas,
    tile, back, first, second, after_first, load_sem, pair_sems, near_sems, first_sent, passed,
    recv_right, recv_relay, recv_left, recv_y, recv_core, recv_fed, stage_sems,
):
    time, group, core, right, left, across, partner = place()
    count = lax.axis_size("tm")
    from_left = left["mom"]
    from_right = right["mom"]

    def rows(j, count_of=1):
        return pl.ds(pl.multiple_of(j * PIECE_ROWS, PIECE_ROWS), PIECE_ROWS * count_of)

    def remote(src, dst, send, recv, device):
        return pltpu.make_async_remote_copy(
            src_ref=src, dst_ref=dst, send_sem=send, recv_sem=recv, device_id=device, device_id_type=MESH
        )

    def to_right(j, held=own, sent=0, many=1):
        at = rows(j, many)
        return remote(
            held.at[:, :, at, :], source.at[group, :, :, at, :], first_sent.at[sent], recv_right.at[j], right
        )

    def to_left(j, held=own, sent=0, many=1):
        at = rows(j, many)
        return remote(held.at[:, :, at, :], ahead.at[:, :, at, :], first_sent.at[sent], recv_left.at[j // SUB], left)

    def to_relay(j, many=1):
        at = rows(j, many)
        device = {"tm": (time + 3) % count, "mom": right["mom"]}
        return remote(own.at[:, :, at, :], relay.at[:, :, at, :], first_sent.at[2], recv_relay.at[j], device)

    def relay_y(j, many=1):
        at = rows(j, many)
        device = {"tm": partner["tm"], "mom": 1 - group}
        return remote(
            relay.at[:, :, at, :], source.at[from_left, :, :, at, :], passed.at[0], recv_y.at[j // SUB], device
        )

    def relay_core(j, many=1):
        at = rows(j, many)
        return remote(
            relay.at[:, :, at, :], source.at[from_left, :, :, at, :], passed.at[1], recv_core.at[j // SUB], partner
        )

    def over_y(j, many=1):
        part = source.at[from_left, :, :, rows(j, many), :]
        return remote(part, part, passed.at[2], recv_y.at[j // SUB], across)

    def feed_source(j, many=1):
        at = rows(j, many)
        return remote(source.at[from_left, :, :, at, :], fed.at[:, :, at, :], passed.at[3], recv_fed.at[0], partner)

    def feed_ahead(j, many=1):
        at = rows(j, many)
        return remote(ahead.at[:, :, at, :], fed.at[:, :, at, :], passed.at[3], recv_fed.at[0], partner)

    nearly = PIECES - SUB // 2
    near_copy = remote(fields, near, near_sems.at[0], near_sems.at[1], partner)
    pair_copy = remote(pairs, pairs_in, pair_sems.at[0], pair_sems.at[1], across)
    load = pltpu.make_async_copy(fields, own, load_sem)

    level = time // 8 % 8
    place_in_level = (time // 64 * 2 + group) * 8 + time % 8
    in_level = [(place_in_level + d) % LEVEL_DEVICES for d in range(1, LEVEL_DEVICES)]
    in_column = [(level + d) % LEVELS for d in range(1, LEVELS)]
    level_devices = [{"tm": n // 16 * 64 + level * 8 + n % 8, "mom": n // 8 % 2} for n in in_level]
    column_devices = [{"tm": time + (n - level) * 8, "mom": group} for n in in_column]
    back_devices = [{"tm": (time + count - 2) % count, "mom": h} for h in range(2)]
    behind_devices = [{"tm": (time + 2) % count, "mom": h} for h in range(2)]

    barrier = pltpu.get_barrier_semaphore()
    relays = [
        {"tm": (time + count + 3 - 6 * core) % count, "mom": jnp.where(core == 0, right["mom"], left["mom"])},
    ]
    greeted = column_devices + level_devices + back_devices + behind_devices + relays
    for device in greeted:
        pl.semaphore_signal(barrier, inc=1, device_id=device, device_id_type=MESH)
    own_tables = [
        pltpu.make_async_copy(pairs, pairs_own, pair_sems.at[2]),
        pltpu.make_async_copy(deltas_in, deltas, pair_sems.at[3]),
    ]
    load.start()
    for copy in own_tables:
        copy.start()
    pl.semaphore_wait(barrier, len(greeted))

    @pl.when(core == 1)
    def _():
        @pl.loop(0, PIECES)
        def _(j):
            to_right(j, fields, j // nearly).start()

    @pl.when(core == 0)
    def _():
        @pl.loop(0, PIECES)
        def _(j):
            to_left(j, fields, j // nearly).start()

    pair_copy.start()
    near_copy.start()

    @pl.loop(0, SEPS * PAIRS)
    def _(i):
        boxes[i] = jnp.zeros((8, 128), jnp.float32)
        directs[i] = jnp.zeros((8, 128), jnp.float32)

        @pl.loop(0, NEV // 32)
        def _(r):
            at = pl.ds(pl.multiple_of(r * 32, 32), 32)
            sums[i, at, :] = jnp.zeros((32, NEV), jnp.float32)
            flips[i, at, :] = jnp.zeros((32, NEV), jnp.float32)

    rows_out[...] = jnp.zeros_like(rows_out)
    load.wait()
    for copy in own_tables:
        copy.wait()
    pair_copy.wait_recv()
    pair_load = pltpu.make_async_copy(pairs_in, pairs_other, load_sem)
    pair_load.start()
    pair_load.wait()

    def pair(of_group, which, side):
        return jnp.where(of_group == group, pairs_own[side, which], pairs_other[side, which])

    def widen(n):
        at = pl.ds(pl.multiple_of(n * ROWS, ROWS), ROWS)
        for momentum in range(4):
            real = source[momentum // 2, momentum % 2, 0, at, :]
            imag = source[momentum // 2, momentum % 2, 1, at, :]
            wide[momentum, n, :ROWS, :NEV] = real
            wide[momentum, n, :ROWS, NEV:] = -imag
            wide[momentum, n, ROWS:, :NEV] = imag
            wide[momentum, n, ROWS:, NEV:] = real

    def work(targets, n):
        at = pl.ds(pl.multiple_of(n * ROWS, ROWS), ROWS)
        diagonal = (
            lax.broadcasted_iota(jnp.int32, (ROWS, NEV), 0) + n * ROWS
            == lax.broadcasted_iota(jnp.int32, (ROWS, NEV), 1)
        )
        for slot, target, of_group in targets:
            for which in range(PAIRS):
                i = slot * PAIRS + which
                a = pair(of_group, which, 0)
                b = lax.rem(pair(of_group, which, 1), 2)
                full = jnp.dot(
                    wide[a, n], target[b].reshape(2 * NEV, NEV), preferred_element_type=jnp.float32
                )
                real, imag = full[:ROWS], full[ROWS:]
                plus = real + imag
                flipped = (real - imag).T
                box = folded(plus * flips[i, at, :])
                sums[i, at, :] = plus
                flips[i, :, at] = flipped
                boxes[i] += box + folded(sums[i, :, at] * flipped)
                directs[i] += folded(jnp.where(diagonal, real, 0.0))

    fed_group = jnp.where(core == 0, from_left, from_right)
    own_part, near_part = (0, own, group), (1, near, group)
    fed_part, ahead_part = (2, fed, fed_group), (3, ahead, from_right)

    @pl.when(core == 0)
    def _():
        to_left(0, many=nearly).wait_send()

        @pl.loop(0, PIECES)
        def _(j):
            to_relay(j).start()

        @pl.loop(0, CHUNKS)
        def _(n):
            to_left(n * SUB, many=SUB).wait_recv()
            feed_ahead(n * SUB, SUB).start()

        feed_source(0, PIECES).wait_recv()
        near_copy.wait_recv()

        @pl.loop(0, CHUNKS)
        def _(n):
            relay_core(n * SUB, SUB).wait_recv()
            relay_y(n * SUB, SUB).wait_recv()
            widen(n)
            work([own_part, near_part, fed_part, ahead_part], n)

    @pl.when(core == 1)
    def _():
        @pl.loop(0, 2 * CHUNKS)
        def _(step):
            for q in range(SUB):

                @pl.when(step < CHUNKS)
                def _():
                    j = step * SUB + q
                    to_right(j).wait_recv()
                    over_y(j).start()
                    feed_source(j).start()

                @pl.when(step >= CHUNKS)
                def _():
                    j = (step - CHUNKS) * SUB + q
                    to_relay(j).wait_recv()
                    relay_y(j).start()
                    relay_core(j).start()

                if q == 1:

                    @pl.when(step == CHUNKS - 1)
                    def _():
                        to_right(0, many=nearly).wait_send()

                        @pl.loop(0, PIECES)
                        def _(j):
                            to_left(j, sent=2).start()

                if q == 2:

                    @pl.when(step == 1)
                    def _():
                        near_copy.wait_recv()

                    @pl.when((step >= 1) & (step <= CHUNKS))
                    def _():
                        over_y((step - 1) * SUB, SUB).wait_recv()
                        widen(step - 1)
                        work([own_part, near_part], step - 1)

                if q == 0:

                    @pl.when(step == CHUNKS + 1)
                    def _():
                        feed_ahead(0, PIECES).wait_recv()

                        @pl.loop(0, CHUNKS // 2)
                        def _(n):
                            work([fed_part], n)

                    @pl.when(step == CHUNKS + 2)
                    def _():
                        @pl.loop(CHUNKS // 2, CHUNKS)
                        def _(n):
                            work([fed_part], n)

        @pl.loop(0, CHUNKS)
        def _(n):
            to_left(n * SUB, many=SUB).wait_recv()

        @pl.loop(0, CHUNKS)
        def _(n):
            work([ahead_part], n)

    separations = (1, 2 - 2 * core, 2 * core, 3)
    groups = (group, group, fed_group, from_right)
    lane = lax.broadcasted_iota(jnp.int32, (8, 128), 1)
    wanted = functools.reduce(
        jnp.add, [jnp.where(lane % SEPS == r, deltas[r], 0) for r in range(SEPS)]
    )
    for slot in range(SEPS):
        for kind, values in enumerate((directs, boxes)):
            for which in range(PAIRS):
                line = slot * 8 + which * 2 + kind
                rows_out[line : line + 1, :] = values[slot * PAIRS + which].sum(0, keepdims=True)
    totals = jnp.broadcast_to(rows_out[...].sum(1, keepdims=True), rows_out.shape)
    tile[...] = functools.reduce(
        jnp.add,
        [
            jnp.where(
                (wanted == separations[slot]) & (lane // SEPS == groups[slot]), totals[slot * 8 : slot * 8 + 8], 0.0
            )
            for slot in range(SEPS)
        ],
    )

    returns = [
        remote(tile, back.at[group], stage_sems.at[0], stage_sems.at[1], device) for device in back_devices
    ]
    for copy in returns:
        copy.start()

    def sent():
        @pl.when(core == 0)
        def _():
            to_left(nearly, sent=1, many=PIECES - nearly).wait_send()
            to_relay(0, PIECES).wait_send()
            feed_ahead(0, PIECES).wait_send()

        @pl.when(core == 1)
        def _():
            to_right(nearly, sent=1, many=PIECES - nearly).wait_send()
            to_left(0, sent=2, many=PIECES).wait_send()
            over_y(0, PIECES).wait_send()
            feed_source(0, PIECES).wait_send()
            relay_y(0, PIECES).wait_send()
            relay_core(0, PIECES).wait_send()

        near_copy.wait_send()
        pair_copy.wait_send()

    def stage(src, held, mine, devices, sems):
        for device in devices:
            remote(src, held.at[mine], stage_sems.at[sems], stage_sems.at[sems + 1], device).start()
        held[mine] = src[...]
        if held is first:
            sent()
        arrived = held.at[: len(devices)]
        all_of_them = remote(arrived, arrived, stage_sems.at[sems], stage_sems.at[sems + 1], devices[0])
        all_of_them.wait_recv()
        return all_of_them, functools.reduce(jnp.add, [held[i] for i in range(held.shape[0])])

    def deliver(values, out):
        mine = jnp.where(group == 0, values[:, :SEPS], values[:, SEPS : 2 * SEPS])
        for which in range(PAIRS):
            results[out, which] = mine[which * 2 : which * 2 + 2]

    copies_1, value = stage(tile, first, place_in_level, level_devices, 2)
    after_first[...] = value
    copies_2, value = stage(after_first, second, level, column_devices, 4)
    deliver(value, 1)
    both = remote(back, back, stage_sems.at[0], stage_sems.at[1], back_devices[0])
    both.wait_recv()
    deliver(back[0] + back[1], 0)
    for copies in (both, copies_1, copies_2):
        copies.wait_send()


def per_device(fields, mom_pairs, deltas):
    field = (2, 2, NEV, NEV)
    dma = pltpu.SemaphoreType.DMA
    results = pl.pallas_call(
        trace_kernel,
        out_shape=pltpu.VMEM((2, PAIRS, 2, SEPS), jnp.float32),
        in_specs=[
            pl.BlockSpec(memory_space=pl.ANY),
            pl.BlockSpec(memory_space=pl.ANY),
            pl.BlockSpec(memory_space=pl.ANY),
        ],
        out_specs=pl.BlockSpec(memory_space=pltpu.VMEM),
        scratch_shapes=[
            pltpu.VMEM(field, jnp.bfloat16),
            pltpu.VMEM(field, jnp.bfloat16),
            pltpu.VMEM(field, jnp.bfloat16),
            pltpu.VMEM(field, jnp.bfloat16),
            pltpu.VMEM(field, jnp.bfloat16),
            pltpu.VMEM((2, *field), jnp.bfloat16),
            pltpu.VMEM((4, CHUNKS, 2 * ROWS, 2 * NEV), jnp.bfloat16),
            pltpu.VMEM((SEPS * PAIRS, NEV, NEV), jnp.float32),
            pltpu.VMEM((SEPS * PAIRS, NEV, NEV), jnp.float32),
            pltpu.VMEM((SEPS * PAIRS, 8, 128), jnp.float32),
            pltpu.VMEM((SEPS * PAIRS, 8, 128), jnp.float32),
            pltpu.VMEM((SEPS * 8, 128), jnp.float32),
            pltpu.VMEM((2, PAIRS), jnp.int32),
            pltpu.SMEM((2, PAIRS), jnp.int32),
            pltpu.SMEM((2, PAIRS), jnp.int32),
            pltpu.SMEM((SEPS,), jnp.int32),
            pltpu.VMEM((8, 128), jnp.float32),
            pltpu.VMEM((2, 8, 128), jnp.float32),
            pltpu.VMEM((LEVEL_DEVICES, 8, 128), jnp.float32),
            pltpu.VMEM((LEVELS, 8, 128), jnp.float32),
            pltpu.VMEM((8, 128), jnp.float32),
            dma,
        ]
        + [dma((n,)) for n in (4, 2, 3, 4, PIECES, PIECES, CHUNKS, CHUNKS, CHUNKS, 1, 6)],
        compiler_params=pltpu.CompilerParams(
            collective_id=0, has_side_effects=True, vmem_limit_bytes=62 * 1024 * 1024
        ),
        name="traces",
    )(mom_pairs.T, deltas, fields.reshape(field))
    times, total = results.transpose(0, 2, 3, 1)
    return times[None], total


def solution(mesh):
    return jax.shard_map(
        per_device,
        mesh=mesh,
        in_specs=(P("tm", "mom", None, None, None), P("mom", None), P()),
        out_specs=(P("tm", None, None, "mom"), P(None, None, "mom")),
        check_vma=False,
    )
```

```python
import functools

import jax
import jax.numpy as jnp
from jax import lax
from jax.experimental import pallas as pl
from jax.experimental.pallas import tpu as pltpu
from jax.sharding import PartitionSpec as P

MESH = pl.DeviceIdType.MESH
CHIPS_PER_PLANE = 32
ROWS = 128
CHUNKS = 4
LEVELS, LEVEL_DEVICES = 8, 32
SUB = 4
PIECES = CHUNKS * SUB
PIECE_ROWS = ROWS // SUB
NEV = ROWS * CHUNKS
PAIRS = 3
SEPS = 4


def place():
    time, group = lax.axis_index("tm"), lax.axis_index("mom")
    count = lax.axis_size("tm")
    chip, core = time // 2, time % 2
    swap_right = (chip % CHIPS_PER_PLANE) // (CHIPS_PER_PLANE - 1)
    swap_left = ((chip + 1) % CHIPS_PER_PLANE == 1).astype(jnp.int32)
    right = {"tm": (time + 2) % count, "mom": (group + swap_right) % 2}
    left = {"tm": (time + count - 2) % count, "mom": (group + swap_left) % 2}
    across = {"tm": time, "mom": 1 - group}
    partner = {"tm": time + 1 - 2 * core, "mom": group}
    return time, group, core, right, left, across, partner


def folded(values):
    total = values.reshape(-1, 8, values.shape[-1]).sum(0)
    lanes = [total[:, i : i + 128] for i in range(0, values.shape[-1], 128)]
    return functools.reduce(jnp.add, lanes)


def trace_kernel(
    pairs, deltas_in, fields, results,
    own, near, fed, ahead, relay, spare, relay_spare, source, wide, sums, flips, boxes, directs, rows_out, pairs_in, pairs_own, pairs_other, deltas,
    tile, back, first, second, after_first, load_sem, pair_sems, near_sems, first_sent, passed,
    recv_right, recv_relay, recv_left, recv_y, recv_core, recv_fed, stage_sems, spare_sems,
):
    time, group, core, right, left, across, partner = place()
    count = lax.axis_size("tm")
    from_left = left["mom"]
    from_right = right["mom"]

    def rows(j, count_of=1):
        return pl.ds(pl.multiple_of(j * PIECE_ROWS, PIECE_ROWS), PIECE_ROWS * count_of)

    def remote(src, dst, send, recv, device):
        return pltpu.make_async_remote_copy(
            src_ref=src, dst_ref=dst, send_sem=send, recv_sem=recv, device_id=device, device_id_type=MESH
        )

    def to_right(j, sent=0, many=1):
        at = rows(j, many)
        return remote(
            own.at[:, :, at, :], source.at[group, :, :, at, :], first_sent.at[sent], recv_right.at[j], right
        )

    def to_left(j, sent=0, many=1):
        at = rows(j, many)
        return remote(own.at[:, :, at, :], ahead.at[:, :, at, :], first_sent.at[sent], recv_left.at[j // SUB], left)

    def to_relay(j, many=1):
        at = rows(j, many)
        device = {"tm": (time + 3) % count, "mom": right["mom"]}
        return remote(own.at[:, :, at, :], relay.at[:, :, at, :], first_sent.at[2], recv_relay.at[j], device)

    def relay_y(j, many=1):
        at = rows(j, many)
        device = {"tm": partner["tm"], "mom": 1 - group}
        return remote(
            relay.at[:, :, at, :], source.at[from_left, :, :, at, :], passed.at[0], recv_y.at[j // SUB], device
        )

    def relay_core(j, many=1):
        at = rows(j, many)
        return remote(
            relay.at[:, :, at, :], source.at[from_left, :, :, at, :], passed.at[1], recv_core.at[j // SUB], partner
        )

    def over_y(j, many=1):
        part = source.at[from_left, :, :, rows(j, many), :]
        return remote(part, part, passed.at[2], recv_y.at[j // SUB], across)

    def feed_source(j, many=1):
        at = rows(j, many)
        return remote(source.at[from_left, :, :, at, :], fed.at[:, :, at, :], passed.at[3], recv_fed.at[0], partner)

    def feed_ahead(j, many=1):
        at = rows(j, many)
        return remote(ahead.at[:, :, at, :], fed.at[:, :, at, :], passed.at[3], recv_fed.at[0], partner)

    nearly = PIECES - SUB // 2
    last = PIECES - 1
    spare_copy = remote(own.at[:, :, rows(last), :], spare, spare_sems.at[0], spare_sems.at[1], across)
    spare_right = remote(
        spare, relay_spare, spare_sems.at[2], spare_sems.at[3], {"tm": (time + 3) % count, "mom": right["mom"]}
    )
    spare_core = remote(
        relay_spare, source.at[1 - from_left, :, :, rows(last), :], spare_sems.at[4], spare_sems.at[5], partner
    )
    near_copy = remote(own, near, near_sems.at[0], near_sems.at[1], partner)
    pair_copy = remote(pairs, pairs_in, pair_sems.at[0], pair_sems.at[1], across)
    load = pltpu.make_async_copy(fields, own, load_sem)

    level = time // 8 % 8
    place_in_level = (time // 64 * 2 + group) * 8 + time % 8
    in_level = [(place_in_level + d) % LEVEL_DEVICES for d in range(1, LEVEL_DEVICES)]
    in_column = [(level + d) % LEVELS for d in range(1, LEVELS)]
    level_devices = [{"tm": n // 16 * 64 + level * 8 + n % 8, "mom": n // 8 % 2} for n in in_level]
    column_devices = [{"tm": time + (n - level) * 8, "mom": group} for n in in_column]
    back_devices = [{"tm": (time + count - 2) % count, "mom": h} for h in range(2)]
    behind_devices = [{"tm": (time + 2) % count, "mom": h} for h in range(2)]

    barrier = pltpu.get_barrier_semaphore()
    relays = [
        {"tm": (time + count + 3 - 6 * core) % count, "mom": jnp.where(core == 0, right["mom"], left["mom"])},
    ]
    greeted = column_devices + level_devices + back_devices + behind_devices + relays
    for device in greeted:
        pl.semaphore_signal(barrier, inc=1, device_id=device, device_id_type=MESH)
    own_tables = [
        pltpu.make_async_copy(pairs, pairs_own, pair_sems.at[2]),
        pltpu.make_async_copy(deltas_in, deltas, pair_sems.at[3]),
    ]
    load.start()
    for copy in own_tables:
        copy.start()
    load.wait()
    pl.semaphore_wait(barrier, len(greeted))

    @pl.when(core == 1)
    def _():
        @pl.loop(0, PIECES)
        def _(j):
            to_right(j, j // nearly).start()

    @pl.when(core == 0)
    def _():
        @pl.loop(0, PIECES)
        def _(j):
            to_left(j, j // nearly).start()

        spare_copy.start()

    pair_copy.start()
    near_copy.start()

    @pl.loop(0, SEPS * PAIRS)
    def _(i):
        boxes[i] = jnp.zeros((8, 128), jnp.float32)
        directs[i] = jnp.zeros((8, 128), jnp.float32)

        @pl.loop(0, NEV // 32)
        def _(r):
            at = pl.ds(pl.multiple_of(r * 32, 32), 32)
            sums[i, at, :] = jnp.zeros((32, NEV), jnp.float32)
            flips[i, at, :] = jnp.zeros((32, NEV), jnp.float32)

    rows_out[...] = jnp.zeros_like(rows_out)
    for copy in own_tables:
        copy.wait()
    pair_copy.wait_recv()
    pair_load = pltpu.make_async_copy(pairs_in, pairs_other, load_sem)
    pair_load.start()
    pair_load.wait()

    def pair(of_group, which, side):
        return jnp.where(of_group == group, pairs_own[side, which], pairs_other[side, which])

    def widen(n):
        at = pl.ds(pl.multiple_of(n * ROWS, ROWS), ROWS)
        for momentum in range(4):
            real = source[momentum // 2, momentum % 2, 0, at, :]
            imag = source[momentum // 2, momentum % 2, 1, at, :]
            wide[momentum, n, :ROWS, :NEV] = real
            wide[momentum, n, :ROWS, NEV:] = -imag
            wide[momentum, n, ROWS:, :NEV] = imag
            wide[momentum, n, ROWS:, NEV:] = real

    def work(targets, n):
        at = pl.ds(pl.multiple_of(n * ROWS, ROWS), ROWS)
        diagonal = (
            lax.broadcasted_iota(jnp.int32, (ROWS, NEV), 0) + n * ROWS
            == lax.broadcasted_iota(jnp.int32, (ROWS, NEV), 1)
        )
        for slot, target, of_group in targets:
            for which in range(PAIRS):
                i = slot * PAIRS + which
                a = pair(of_group, which, 0)
                b = lax.rem(pair(of_group, which, 1), 2)
                full = jnp.dot(
                    wide[a, n], target[b].reshape(2 * NEV, NEV), preferred_element_type=jnp.float32
                )
                real, imag = full[:ROWS], full[ROWS:]
                plus = real + imag
                flipped = (real - imag).T
                box = folded(plus * flips[i, at, :])
                sums[i, at, :] = plus
                flips[i, :, at] = flipped
                boxes[i] += box + folded(sums[i, :, at] * flipped)
                directs[i] += folded(jnp.where(diagonal, real, 0.0))

    fed_group = jnp.where(core == 0, from_left, from_right)
    own_part, near_part = (0, own, group), (1, near, group)
    fed_part, ahead_part = (2, fed, fed_group), (3, ahead, from_right)

    @pl.when(core == 0)
    def _():
        to_left(0, many=nearly).wait_send()

        @pl.loop(0, PIECES)
        def _(j):
            to_relay(j).start()

        spare_copy.wait_recv()
        spare_right.start()

        @pl.loop(0, CHUNKS)
        def _(n):
            to_left(n * SUB, many=SUB).wait_recv()
            feed_ahead(n * SUB, SUB).start()

        feed_source(0, PIECES).wait_recv()
        near_copy.wait_recv()

        @pl.loop(0, CHUNKS)
        def _(n):
            relay_core(n * SUB, SUB).wait_recv()

            @pl.when(n < CHUNKS - 1)
            def _():
                relay_y(n * SUB, SUB).wait_recv()

            @pl.when(n == CHUNKS - 1)
            def _():
                relay_y(last + 1 - SUB, SUB - 1).wait_recv()
                spare_core.wait_recv()

            widen(n)
            work([own_part, near_part, fed_part, ahead_part], n)

    @pl.when(core == 1)
    def _():
        @pl.loop(0, 2 * CHUNKS)
        def _(step):
            for q in range(SUB):

                @pl.when(step < CHUNKS)
                def _():
                    j = step * SUB + q
                    to_right(j).wait_recv()
                    over_y(j).start()
                    feed_source(j).start()

                @pl.when(step >= CHUNKS)
                def _():
                    j = (step - CHUNKS) * SUB + q
                    to_relay(j).wait_recv()
                    relay_core(j).start()

                    @pl.when(j < last)
                    def _():
                        relay_y(j).start()

                if q == 1:

                    @pl.when(step == CHUNKS - 1)
                    def _():
                        to_right(0, many=nearly).wait_send()

                        @pl.loop(0, PIECES)
                        def _(j):
                            to_left(j, sent=2).start()

                if q == 2:

                    @pl.when(step == 1)
                    def _():
                        near_copy.wait_recv()

                    @pl.when((step >= 1) & (step <= CHUNKS))
                    def _():
                        over_y((step - 1) * SUB, SUB).wait_recv()
                        widen(step - 1)
                        work([own_part, near_part], step - 1)

                if q == 0:

                    @pl.when(step == CHUNKS + 1)
                    def _():
                        feed_ahead(0, PIECES).wait_recv()

                        @pl.loop(0, CHUNKS // 2)
                        def _(n):
                            work([fed_part], n)

                    @pl.when(step == CHUNKS + 2)
                    def _():
                        @pl.loop(CHUNKS // 2, CHUNKS)
                        def _(n):
                            work([fed_part], n)

        spare_right.wait_recv()
        spare_core.start()

        @pl.loop(0, CHUNKS)
        def _(n):
            to_left(n * SUB, many=SUB).wait_recv()

        @pl.loop(0, CHUNKS)
        def _(n):
            work([ahead_part], n)

    separations = (1, 2 - 2 * core, 2 * core, 3)
    groups = (group, group, fed_group, from_right)
    lane = lax.broadcasted_iota(jnp.int32, (8, 128), 1)
    wanted = functools.reduce(
        jnp.add, [jnp.where(lane % SEPS == r, deltas[r], 0) for r in range(SEPS)]
    )
    for slot in range(SEPS):
        for kind, values in enumerate((directs, boxes)):
            for which in range(PAIRS):
                line = slot * 8 + which * 2 + kind
                rows_out[line : line + 1, :] = values[slot * PAIRS + which].sum(0, keepdims=True)
    totals = jnp.broadcast_to(rows_out[...].sum(1, keepdims=True), rows_out.shape)
    tile[...] = functools.reduce(
        jnp.add,
        [
            jnp.where(
                (wanted == separations[slot]) & (lane // SEPS == groups[slot]), totals[slot * 8 : slot * 8 + 8], 0.0
            )
            for slot in range(SEPS)
        ],
    )

    returns = [
        remote(tile, back.at[group], stage_sems.at[0], stage_sems.at[1], device) for device in back_devices
    ]
    for copy in returns:
        copy.start()

    def sent():
        @pl.when(core == 0)
        def _():
            to_left(nearly, sent=1, many=PIECES - nearly).wait_send()
            to_relay(0, PIECES).wait_send()
            spare_copy.wait_send()
            spare_right.wait_send()
            feed_ahead(0, PIECES).wait_send()

        @pl.when(core == 1)
        def _():
            to_right(nearly, sent=1, many=PIECES - nearly).wait_send()
            to_left(0, sent=2, many=PIECES).wait_send()
            over_y(0, PIECES).wait_send()
            feed_source(0, PIECES).wait_send()
            relay_y(0, last).wait_send()
            spare_core.wait_send()
            relay_core(0, PIECES).wait_send()

        near_copy.wait_send()
        pair_copy.wait_send()

    def stage(src, held, mine, devices, sems):
        for device in devices:
            remote(src, held.at[mine], stage_sems.at[sems], stage_sems.at[sems + 1], device).start()
        held[mine] = src[...]
        if held is first:
            sent()
        arrived = held.at[: len(devices)]
        all_of_them = remote(arrived, arrived, stage_sems.at[sems], stage_sems.at[sems + 1], devices[0])
        all_of_them.wait_recv()
        return all_of_them, functools.reduce(jnp.add, [held[i] for i in range(held.shape[0])])

    def deliver(values, out):
        mine = jnp.where(group == 0, values[:, :SEPS], values[:, SEPS : 2 * SEPS])
        for which in range(PAIRS):
            results[out, which] = mine[which * 2 : which * 2 + 2]

    copies_1, value = stage(tile, first, place_in_level, level_devices, 2)
    after_first[...] = value
    copies_2, value = stage(after_first, second, level, column_devices, 4)
    deliver(value, 1)
    both = remote(back, back, stage_sems.at[0], stage_sems.at[1], back_devices[0])
    both.wait_recv()
    deliver(back[0] + back[1], 0)
    for copies in (both, copies_1, copies_2):
        copies.wait_send()


def per_device(fields, mom_pairs, deltas):
    field = (2, 2, NEV, NEV)
    dma = pltpu.SemaphoreType.DMA
    results = pl.pallas_call(
        trace_kernel,
        out_shape=pltpu.VMEM((2, PAIRS, 2, SEPS), jnp.float32),
        in_specs=[
            pl.BlockSpec(memory_space=pl.ANY),
            pl.BlockSpec(memory_space=pl.ANY),
            pl.BlockSpec(memory_space=pl.ANY),
        ],
        out_specs=pl.BlockSpec(memory_space=pltpu.VMEM),
        scratch_shapes=[
            pltpu.VMEM(field, jnp.bfloat16),
            pltpu.VMEM(field, jnp.bfloat16),
            pltpu.VMEM(field, jnp.bfloat16),
            pltpu.VMEM(field, jnp.bfloat16),
            pltpu.VMEM(field, jnp.bfloat16),
            pltpu.VMEM((2, 2, PIECE_ROWS, NEV), jnp.bfloat16),
            pltpu.VMEM((2, 2, PIECE_ROWS, NEV), jnp.bfloat16),
            pltpu.VMEM((2, *field), jnp.bfloat16),
            pltpu.VMEM((4, CHUNKS, 2 * ROWS, 2 * NEV), jnp.bfloat16),
            pltpu.VMEM((SEPS * PAIRS, NEV, NEV), jnp.float32),
            pltpu.VMEM((SEPS * PAIRS, NEV, NEV), jnp.float32),
            pltpu.VMEM((SEPS * PAIRS, 8, 128), jnp.float32),
            pltpu.VMEM((SEPS * PAIRS, 8, 128), jnp.float32),
            pltpu.VMEM((SEPS * 8, 128), jnp.float32),
            pltpu.VMEM((2, PAIRS), jnp.int32),
            pltpu.SMEM((2, PAIRS), jnp.int32),
            pltpu.SMEM((2, PAIRS), jnp.int32),
            pltpu.SMEM((SEPS,), jnp.int32),
            pltpu.VMEM((8, 128), jnp.float32),
            pltpu.VMEM((2, 8, 128), jnp.float32),
            pltpu.VMEM((LEVEL_DEVICES, 8, 128), jnp.float32),
            pltpu.VMEM((LEVELS, 8, 128), jnp.float32),
            pltpu.VMEM((8, 128), jnp.float32),
            dma,
        ]
        + [dma((n,)) for n in (4, 2, 3, 4, PIECES, PIECES, CHUNKS, CHUNKS, CHUNKS, 1, 6, 6)],
        compiler_params=pltpu.CompilerParams(
            collective_id=0, has_side_effects=True, vmem_limit_bytes=62 * 1024 * 1024
        ),
        name="traces",
    )(mom_pairs.T, deltas, fields.reshape(field))
    times, total = results.transpose(0, 2, 3, 1)
    return times[None], total


def solution(mesh):
    return jax.shard_map(
        per_device,
        mesh=mesh,
        in_specs=(P("tm", "mom", None, None, None), P("mom", None), P()),
        out_specs=(P("tm", None, None, "mom"), P(None, None, "mom")),
        check_vma=False,
    )
```

```python
import functools

import jax
import jax.numpy as jnp
from jax import lax
from jax.experimental import pallas as pl
from jax.experimental.pallas import tpu as pltpu
from jax.sharding import PartitionSpec as P

MESH = pl.DeviceIdType.MESH
CHIPS_PER_PLANE = 32
ROWS = 128
CHUNKS = 4
LEVELS, LEVEL_DEVICES = 8, 32
SUB = 4
PIECES = CHUNKS * SUB
PIECE_ROWS = ROWS // SUB
NEV = ROWS * CHUNKS
PAIRS = 3
SEPS = 4


def place():
    time, group = lax.axis_index("tm"), lax.axis_index("mom")
    count = lax.axis_size("tm")
    chip, core = time // 2, time % 2
    swap_right = (chip % CHIPS_PER_PLANE) // (CHIPS_PER_PLANE - 1)
    swap_left = ((chip + 1) % CHIPS_PER_PLANE == 1).astype(jnp.int32)
    right = {"tm": (time + 2) % count, "mom": (group + swap_right) % 2}
    left = {"tm": (time + count - 2) % count, "mom": (group + swap_left) % 2}
    across = {"tm": time, "mom": 1 - group}
    partner = {"tm": time + 1 - 2 * core, "mom": group}
    return time, group, core, right, left, across, partner


def folded(values):
    total = values.reshape(-1, 8, values.shape[-1]).sum(0)
    lanes = [total[:, i : i + 128] for i in range(0, values.shape[-1], 128)]
    return functools.reduce(jnp.add, lanes)


def trace_kernel(
    pairs, deltas_in, fields, results,
    own, near, fed, ahead, relay, spare, relay_spare, source, wide, sums, flips, boxes, directs, rows_out, pairs_in, pairs_own, pairs_other, deltas,
    tile, back, first, second, after_first, load_sem, pair_sems, near_sems, first_sent, passed,
    recv_right, recv_relay, recv_left, recv_y, recv_core, recv_fed, stage_sems, spare_sems,
):
    time, group, core, right, left, across, partner = place()
    count = lax.axis_size("tm")
    from_left = left["mom"]
    from_right = right["mom"]

    def rows(j, count_of=1):
        return pl.ds(pl.multiple_of(j * PIECE_ROWS, PIECE_ROWS), PIECE_ROWS * count_of)

    def remote(src, dst, send, recv, device):
        return pltpu.make_async_remote_copy(
            src_ref=src, dst_ref=dst, send_sem=send, recv_sem=recv, device_id=device, device_id_type=MESH
        )

    def to_right(j, sent=0, many=1):
        at = rows(j, many)
        return remote(
            own.at[:, :, at, :], source.at[group, :, :, at, :], first_sent.at[sent], recv_right.at[j], right
        )

    def to_left(j, sent=0, many=1):
        at = rows(j, many)
        return remote(own.at[:, :, at, :], ahead.at[:, :, at, :], first_sent.at[sent], recv_left.at[j // SUB], left)

    def to_relay(j, many=1):
        at = rows(j, many)
        device = {"tm": (time + 3) % count, "mom": right["mom"]}
        return remote(own.at[:, :, at, :], relay.at[:, :, at, :], first_sent.at[2], recv_relay.at[j], device)

    def relay_y(j, many=1):
        at = rows(j, many)
        device = {"tm": partner["tm"], "mom": 1 - group}
        return remote(
            relay.at[:, :, at, :], source.at[from_left, :, :, at, :], passed.at[0], recv_y.at[j // SUB], device
        )

    def relay_core(j, many=1):
        at = rows(j, many)
        return remote(
            relay.at[:, :, at, :], source.at[from_left, :, :, at, :], passed.at[1], recv_core.at[j // SUB], partner
        )

    def over_y(j, many=1):
        part = source.at[from_left, :, :, rows(j, many), :]
        return remote(part, part, passed.at[2], recv_y.at[j // SUB], across)

    def feed_source(j, many=1):
        at = rows(j, many)
        return remote(source.at[from_left, :, :, at, :], fed.at[:, :, at, :], passed.at[3], recv_fed.at[0], partner)

    def feed_ahead(j, many=1):
        at = rows(j, many)
        return remote(ahead.at[:, :, at, :], fed.at[:, :, at, :], passed.at[3], recv_fed.at[0], partner)

    nearly = PIECES - SUB // 2
    last = PIECES - 1
    spare_copy = remote(own.at[:, :, rows(last), :], spare, spare_sems.at[0], spare_sems.at[1], across)
    spare_right = remote(
        spare, relay_spare, spare_sems.at[2], spare_sems.at[3], {"tm": (time + 3) % count, "mom": right["mom"]}
    )
    spare_core = remote(
        relay_spare, source.at[1 - from_left, :, :, rows(last), :], spare_sems.at[4], spare_sems.at[5], partner
    )
    near_copy = remote(own, near, near_sems.at[0], near_sems.at[1], partner)
    pair_copy = remote(pairs, pairs_in, pair_sems.at[0], pair_sems.at[1], across)
    load = pltpu.make_async_copy(fields, own, load_sem)

    level = time // 8 % 8
    place_in_level = (time // 64 * 2 + group) * 8 + time % 8
    in_level = [(place_in_level + d) % LEVEL_DEVICES for d in range(1, LEVEL_DEVICES)]
    in_column = [(level + d) % LEVELS for d in range(1, LEVELS)]
    level_devices = [{"tm": n // 16 * 64 + level * 8 + n % 8, "mom": n // 8 % 2} for n in in_level]
    column_devices = [{"tm": time + (n - level) * 8, "mom": group} for n in in_column]
    back_devices = [{"tm": (time + count - 2) % count, "mom": h} for h in range(2)]
    behind_devices = [{"tm": (time + 2) % count, "mom": h} for h in range(2)]

    barrier = pltpu.get_barrier_semaphore()
    relays = [
        {"tm": (time + count + 3 - 6 * core) % count, "mom": jnp.where(core == 0, right["mom"], left["mom"])},
    ]
    greeted = column_devices + level_devices + back_devices + behind_devices + relays
    for device in greeted:
        pl.semaphore_signal(barrier, inc=1, device_id=device, device_id_type=MESH)
    own_tables = [
        pltpu.make_async_copy(pairs, pairs_own, pair_sems.at[2]),
        pltpu.make_async_copy(deltas_in, deltas, pair_sems.at[3]),
    ]
    load.start()
    for copy in own_tables:
        copy.start()
    load.wait()
    pl.semaphore_wait(barrier, len(greeted))

    @pl.when(core == 1)
    def _():
        @pl.loop(0, PIECES)
        def _(j):
            to_right(j, j // nearly).start()

    @pl.when(core == 0)
    def _():
        @pl.loop(0, PIECES)
        def _(j):
            to_left(j, j // nearly).start()

        spare_copy.start()

    pair_copy.start()
    near_copy.start()

    @pl.loop(0, SEPS * PAIRS)
    def _(i):
        boxes[i] = jnp.zeros((8, 128), jnp.float32)
        directs[i] = jnp.zeros((8, 128), jnp.float32)

        @pl.loop(0, NEV // 32)
        def _(r):
            at = pl.ds(pl.multiple_of(r * 32, 32), 32)
            sums[i, at, :] = jnp.zeros((32, NEV), jnp.float32)
            flips[i, at, :] = jnp.zeros((32, NEV), jnp.float32)

    rows_out[...] = jnp.zeros_like(rows_out)
    for copy in own_tables:
        copy.wait()
    pair_copy.wait_recv()
    pair_load = pltpu.make_async_copy(pairs_in, pairs_other, load_sem)
    pair_load.start()
    pair_load.wait()

    def pair(of_group, which, side):
        return jnp.where(of_group == group, pairs_own[side, which], pairs_other[side, which])

    def widen(n):
        at = pl.ds(pl.multiple_of(n * ROWS, ROWS), ROWS)
        for momentum in range(4):
            real = source[momentum // 2, momentum % 2, 0, at, :]
            imag = source[momentum // 2, momentum % 2, 1, at, :]
            wide[momentum, n, :ROWS, :NEV] = real
            wide[momentum, n, :ROWS, NEV:] = -imag
            wide[momentum, n, ROWS:, :NEV] = imag
            wide[momentum, n, ROWS:, NEV:] = real

    def work(targets, n):
        at = pl.ds(pl.multiple_of(n * ROWS, ROWS), ROWS)
        diagonal = (
            lax.broadcasted_iota(jnp.int32, (ROWS, NEV), 0) + n * ROWS
            == lax.broadcasted_iota(jnp.int32, (ROWS, NEV), 1)
        )
        for slot, target, of_group in targets:
            for which in range(PAIRS):
                i = slot * PAIRS + which
                a = pair(of_group, which, 0)
                b = lax.rem(pair(of_group, which, 1), 2)
                full = jnp.dot(
                    wide[a, n], target[b].reshape(2 * NEV, NEV), preferred_element_type=jnp.float32
                )
                real, imag = full[:ROWS], full[ROWS:]
                plus = real + imag
                flipped = (real - imag).T
                box = folded(plus * flips[i, at, :])
                sums[i, at, :] = plus
                flips[i, :, at] = flipped
                boxes[i] += box + folded(sums[i, :, at] * flipped)
                directs[i] += folded(jnp.where(diagonal, real, 0.0))

    fed_group = jnp.where(core == 0, from_left, from_right)
    own_part, near_part = (0, own, group), (1, near, group)
    fed_part, ahead_part = (2, fed, fed_group), (3, ahead, from_right)

    @pl.when(core == 0)
    def _():
        to_left(0, many=nearly).wait_send()

        @pl.loop(0, PIECES)
        def _(j):
            to_relay(j).start()

        spare_copy.wait_recv()
        spare_right.start()

        @pl.loop(0, CHUNKS)
        def _(n):
            to_left(n * SUB, many=SUB).wait_recv()
            feed_ahead(n * SUB, SUB).start()

        feed_source(0, PIECES).wait_recv()
        near_copy.wait_recv()

        @pl.loop(0, CHUNKS)
        def _(n):
            relay_core(n * SUB, SUB).wait_recv()

            @pl.when(n < CHUNKS - 1)
            def _():
                relay_y(n * SUB, SUB).wait_recv()

            @pl.when(n == CHUNKS - 1)
            def _():
                relay_y(last + 1 - SUB, SUB - 1).wait_recv()
                spare_core.wait_recv()

            widen(n)
            work([own_part, near_part, fed_part, ahead_part], n)

    @pl.when(core == 1)
    def _():
        @pl.loop(0, 2 * CHUNKS)
        def _(step):
            for q in range(SUB):

                @pl.when(step < CHUNKS)
                def _():
                    j = step * SUB + q
                    to_right(j).wait_recv()
                    over_y(j).start()
                    feed_source(j).start()

                @pl.when(step >= CHUNKS)
                def _():
                    j = (step - CHUNKS) * SUB + q
                    to_relay(j).wait_recv()
                    relay_core(j).start()

                    @pl.when(j < last)
                    def _():
                        relay_y(j).start()

                if q == 1:

                    @pl.when(step == CHUNKS - 1)
                    def _():
                        to_right(0, many=nearly).wait_send()

                        @pl.loop(0, PIECES)
                        def _(j):
                            to_left(j, sent=2).start()

                if q == 2:

                    @pl.when(step == 1)
                    def _():
                        near_copy.wait_recv()

                    @pl.when((step >= 1) & (step <= CHUNKS))
                    def _():
                        over_y((step - 1) * SUB, SUB).wait_recv()
                        widen(step - 1)
                        work([own_part, near_part], step - 1)

                if q == 0:

                    @pl.when(step == CHUNKS + 1)
                    def _():
                        feed_ahead(0, PIECES).wait_recv()

                    @pl.when((step == CHUNKS + 1) | (step == CHUNKS + 2))
                    def _():
                        @pl.loop(0, CHUNKS // 2)
                        def _(n):
                            work([fed_part], (step - CHUNKS - 1) * (CHUNKS // 2) + n)

        spare_right.wait_recv()
        spare_core.start()

        @pl.loop(0, CHUNKS)
        def _(n):
            to_left(n * SUB, many=SUB).wait_recv()

        for n in range(CHUNKS):
            work([ahead_part], n)

    separations = (1, 2 - 2 * core, 2 * core, 3)
    groups = (group, group, fed_group, from_right)
    lane = lax.broadcasted_iota(jnp.int32, (8, 128), 1)
    sublane = lax.broadcasted_iota(jnp.int32, (8, 128), 0)
    wanted = functools.reduce(
        jnp.add, [jnp.where(lane % SEPS == r, deltas[r], 0) for r in range(SEPS)]
    )
    for slot in range(SEPS):
        for kind, values in enumerate((directs, boxes)):
            for which in range(PAIRS):
                line = slot * 8 + which * 2 + kind
                rows_out[line : line + 1, :] = values[slot * PAIRS + which].sum(0, keepdims=True)
    totals = jnp.broadcast_to(rows_out[...].sum(1, keepdims=True), rows_out.shape)
    placed = functools.reduce(
        jnp.add,
        [
            jnp.where(
                (wanted == separations[slot]) & (lane // SEPS % 2 == groups[slot]) & (lane // (2 * SEPS) == sublane),
                totals[slot * 8 : slot * 8 + 8],
                0.0,
            )
            for slot in range(SEPS)
        ],
    )
    tile[...] = placed.sum(0, keepdims=True)

    returns = [
        remote(tile, back.at[group], stage_sems.at[0], stage_sems.at[1], device) for device in back_devices
    ]
    for copy in returns:
        copy.start()

    def sent():
        @pl.when(core == 0)
        def _():
            to_left(nearly, sent=1, many=PIECES - nearly).wait_send()
            to_relay(0, PIECES).wait_send()
            spare_copy.wait_send()
            spare_right.wait_send()
            feed_ahead(0, PIECES).wait_send()

        @pl.when(core == 1)
        def _():
            to_right(nearly, sent=1, many=PIECES - nearly).wait_send()
            to_left(0, sent=2, many=PIECES).wait_send()
            over_y(0, PIECES).wait_send()
            feed_source(0, PIECES).wait_send()
            relay_y(0, last).wait_send()
            spare_core.wait_send()
            relay_core(0, PIECES).wait_send()

        near_copy.wait_send()
        pair_copy.wait_send()

    def stage(src, held, mine, devices, sems):
        for device in devices:
            remote(src, held.at[mine], stage_sems.at[sems], stage_sems.at[sems + 1], device).start()
        held[mine] = src[...]
        if held is first:
            sent()
        arrived = held.at[: len(devices)]
        all_of_them = remote(arrived, arrived, stage_sems.at[sems], stage_sems.at[sems + 1], devices[0])
        all_of_them.wait_recv()
        return all_of_them, functools.reduce(jnp.add, [held[i] for i in range(held.shape[0])])

    def deliver(values, out):
        for which in range(PAIRS):
            for kind in range(2):
                begin = (which * 2 + kind) * 2 * SEPS
                both_groups = values[:, begin : begin + SEPS], values[:, begin + SEPS : begin + 2 * SEPS]
                results[out, which, kind : kind + 1, :] = jnp.where(group == 0, *both_groups)

    copies_1, value = stage(tile, first, place_in_level, level_devices, 2)
    after_first[...] = value
    copies_2, value = stage(after_first, second, level, column_devices, 4)
    deliver(value, 1)
    both = remote(back, back, stage_sems.at[0], stage_sems.at[1], back_devices[0])
    both.wait_recv()
    deliver(back[0] + back[1], 0)
    for copies in (both, copies_1, copies_2):
        copies.wait_send()


def per_device(fields, mom_pairs, deltas):
    field = (2, 2, NEV, NEV)
    dma = pltpu.SemaphoreType.DMA
    results = pl.pallas_call(
        trace_kernel,
        out_shape=pltpu.VMEM((2, PAIRS, 2, SEPS), jnp.float32),
        in_specs=[
            pl.BlockSpec(memory_space=pl.ANY),
            pl.BlockSpec(memory_space=pl.ANY),
            pl.BlockSpec(memory_space=pl.ANY),
        ],
        out_specs=pl.BlockSpec(memory_space=pltpu.VMEM),
        scratch_shapes=[
            pltpu.VMEM(field, jnp.bfloat16),
            pltpu.VMEM(field, jnp.bfloat16),
            pltpu.VMEM(field, jnp.bfloat16),
            pltpu.VMEM(field, jnp.bfloat16),
            pltpu.VMEM(field, jnp.bfloat16),
            pltpu.VMEM((2, 2, PIECE_ROWS, NEV), jnp.bfloat16),
            pltpu.VMEM((2, 2, PIECE_ROWS, NEV), jnp.bfloat16),
            pltpu.VMEM((2, *field), jnp.bfloat16),
            pltpu.VMEM((4, CHUNKS, 2 * ROWS, 2 * NEV), jnp.bfloat16),
            pltpu.VMEM((SEPS * PAIRS, NEV, NEV), jnp.float32),
            pltpu.VMEM((SEPS * PAIRS, NEV, NEV), jnp.float32),
            pltpu.VMEM((SEPS * PAIRS, 8, 128), jnp.float32),
            pltpu.VMEM((SEPS * PAIRS, 8, 128), jnp.float32),
            pltpu.VMEM((SEPS * 8, 128), jnp.float32),
            pltpu.VMEM((2, PAIRS), jnp.int32),
            pltpu.SMEM((2, PAIRS), jnp.int32),
            pltpu.SMEM((2, PAIRS), jnp.int32),
            pltpu.SMEM((SEPS,), jnp.int32),
            pltpu.VMEM((1, 128), jnp.float32),
            pltpu.VMEM((2, 1, 128), jnp.float32),
            pltpu.VMEM((LEVEL_DEVICES, 1, 128), jnp.float32),
            pltpu.VMEM((LEVELS, 1, 128), jnp.float32),
            pltpu.VMEM((1, 128), jnp.float32),
            dma,
        ]
        + [dma((n,)) for n in (4, 2, 3, 4, PIECES, PIECES, CHUNKS, CHUNKS, CHUNKS, 1, 6, 6)],
        compiler_params=pltpu.CompilerParams(
            collective_id=0, has_side_effects=True, vmem_limit_bytes=62 * 1024 * 1024
        ),
        name="traces",
    )(mom_pairs.T, deltas, fields.reshape(field))
    times, total = results.transpose(0, 2, 3, 1)
    return times[None], total


def solution(mesh):
    return jax.shard_map(
        per_device,
        mesh=mesh,
        in_specs=(P("tm", "mom", None, None, None), P("mom", None), P()),
        out_specs=(P("tm", None, None, "mom"), P(None, None, "mom")),
        check_vma=False,
    )
```

```python
import functools

import jax
import jax.numpy as jnp
from jax import lax
from jax.experimental import pallas as pl
from jax.experimental.pallas import tpu as pltpu
from jax.sharding import PartitionSpec as P

MESH = pl.DeviceIdType.MESH
CHIPS_PER_PLANE = 32
ROWS = 128
CHUNKS = 4
LEVELS, LEVEL_DEVICES = 8, 32
SUB = 4
PIECES = CHUNKS * SUB
PIECE_ROWS = ROWS // SUB
NEV = ROWS * CHUNKS
PAIRS = 3
SEPS = 4


def place():
    time, group = lax.axis_index("tm"), lax.axis_index("mom")
    count = lax.axis_size("tm")
    chip, core = time // 2, time % 2
    swap_right = (chip % CHIPS_PER_PLANE) // (CHIPS_PER_PLANE - 1)
    swap_left = ((chip + 1) % CHIPS_PER_PLANE == 1).astype(jnp.int32)
    right = {"tm": (time + 2) % count, "mom": (group + swap_right) % 2}
    left = {"tm": (time + count - 2) % count, "mom": (group + swap_left) % 2}
    across = {"tm": time, "mom": 1 - group}
    partner = {"tm": time + 1 - 2 * core, "mom": group}
    return time, group, core, right, left, across, partner


def folded(values):
    total = values.reshape(-1, 8, values.shape[-1]).sum(0)
    lanes = [total[:, i : i + 128] for i in range(0, values.shape[-1], 128)]
    return functools.reduce(jnp.add, lanes)


def trace_kernel(
    pairs, deltas_in, fields, results,
    own, near, fed, ahead, relay, spare, relay_spare, source, wide, sums, flips, boxes, directs, rows_out, pairs_in, pairs_own, pairs_other, deltas,
    tile, back, first, second, after_first, load_sem, pair_sems, near_sems, first_sent, passed,
    recv_right, recv_relay, recv_left, recv_y, recv_core, recv_fed, stage_sems, spare_sems,
):
    time, group, core, right, left, across, partner = place()
    count = lax.axis_size("tm")
    from_left = left["mom"]
    from_right = right["mom"]

    def rows(j, count_of=1):
        return pl.ds(pl.multiple_of(j * PIECE_ROWS, PIECE_ROWS), PIECE_ROWS * count_of)

    def remote(src, dst, send, recv, device):
        return pltpu.make_async_remote_copy(
            src_ref=src, dst_ref=dst, send_sem=send, recv_sem=recv, device_id=device, device_id_type=MESH
        )

    def to_right(j, sent=0, many=1):
        at = rows(j, many)
        return remote(
            own.at[:, :, at, :], source.at[group, :, :, at, :], first_sent.at[sent], recv_right.at[j], right
        )

    def to_left(j, sent=0, many=1):
        at = rows(j, many)
        return remote(own.at[:, :, at, :], ahead.at[:, :, at, :], first_sent.at[sent], recv_left.at[j // SUB], left)

    def to_relay(j, many=1):
        at = rows(j, many)
        device = {"tm": (time + 3) % count, "mom": right["mom"]}
        return remote(own.at[:, :, at, :], relay.at[:, :, at, :], first_sent.at[2], recv_relay.at[j], device)

    def relay_y(j, many=1):
        at = rows(j, many)
        device = {"tm": partner["tm"], "mom": 1 - group}
        return remote(
            relay.at[:, :, at, :], source.at[from_left, :, :, at, :], passed.at[0], recv_y.at[j // SUB], device
        )

    def relay_core(j, many=1):
        at = rows(j, many)
        return remote(
            relay.at[:, :, at, :], source.at[from_left, :, :, at, :], passed.at[1], recv_core.at[j // SUB], partner
        )

    def over_y(j, many=1):
        part = source.at[from_left, :, :, rows(j, many), :]
        return remote(part, part, passed.at[2], recv_y.at[j // SUB], across)

    def feed_source(j, many=1):
        at = rows(j, many)
        return remote(source.at[from_left, :, :, at, :], fed.at[:, :, at, :], passed.at[3], recv_fed.at[0], partner)

    def feed_ahead(j, many=1):
        at = rows(j, many)
        return remote(ahead.at[:, :, at, :], fed.at[:, :, at, :], passed.at[3], recv_fed.at[0], partner)

    nearly = PIECES - SUB // 2
    last = PIECES - 1
    spare_copy = remote(own.at[:, :, rows(last), :], spare, spare_sems.at[0], spare_sems.at[1], across)
    spare_right = remote(
        spare, relay_spare, spare_sems.at[2], spare_sems.at[3], {"tm": (time + 3) % count, "mom": right["mom"]}
    )
    spare_core = remote(
        relay_spare, source.at[1 - from_left, :, :, rows(last), :], spare_sems.at[4], spare_sems.at[5], partner
    )
    near_copy = remote(own, near, near_sems.at[0], near_sems.at[1], partner)
    pair_copy = remote(pairs, pairs_in, pair_sems.at[0], pair_sems.at[1], across)
    load = pltpu.make_async_copy(fields, own, load_sem)

    level = time // 8 % 8
    place_in_level = (time // 64 * 2 + group) * 8 + time % 8
    in_level = [(place_in_level + d) % LEVEL_DEVICES for d in range(1, LEVEL_DEVICES)]
    in_column = [(level + d) % LEVELS for d in range(1, LEVELS)]
    level_devices = [{"tm": n // 16 * 64 + level * 8 + n % 8, "mom": n // 8 % 2} for n in in_level]
    column_devices = [{"tm": time + (n - level) * 8, "mom": group} for n in in_column]
    back_devices = [{"tm": (time + count - 2) % count, "mom": h} for h in range(2)]
    behind_devices = [{"tm": (time + 2) % count, "mom": h} for h in range(2)]

    barrier = pltpu.get_barrier_semaphore()
    relays = [
        {"tm": (time + count + 3 - 6 * core) % count, "mom": jnp.where(core == 0, right["mom"], left["mom"])},
    ]
    greeted = column_devices + level_devices + back_devices + behind_devices + relays
    for device in greeted:
        pl.semaphore_signal(barrier, inc=1, device_id=device, device_id_type=MESH)
    own_tables = [
        pltpu.make_async_copy(pairs, pairs_own, pair_sems.at[2]),
        pltpu.make_async_copy(deltas_in, deltas, pair_sems.at[3]),
    ]
    load.start()
    for copy in own_tables:
        copy.start()
    load.wait()
    pl.semaphore_wait(barrier, len(greeted))

    @pl.when(core == 1)
    def _():
        @pl.loop(0, PIECES)
        def _(j):
            to_right(j, j // nearly).start()

    @pl.when(core == 0)
    def _():
        @pl.loop(0, PIECES)
        def _(j):
            to_left(j, j // nearly).start()

        spare_copy.start()

    pair_copy.start()
    near_copy.start()

    @pl.loop(0, SEPS * PAIRS)
    def _(i):
        boxes[i] = jnp.zeros((8, 128), jnp.float32)
        directs[i] = jnp.zeros((8, 128), jnp.float32)

        @pl.loop(0, NEV // 32)
        def _(r):
            at = pl.ds(pl.multiple_of(r * 32, 32), 32)
            sums[i, at, :] = jnp.zeros((32, NEV), jnp.float32)
            flips[i, at, :] = jnp.zeros((32, NEV), jnp.float32)

    rows_out[...] = jnp.zeros_like(rows_out)
    for copy in own_tables:
        copy.wait()
    pair_copy.wait_recv()
    pair_load = pltpu.make_async_copy(pairs_in, pairs_other, load_sem)
    pair_load.start()
    pair_load.wait()

    def pair(of_group, which, side):
        return jnp.where(of_group == group, pairs_own[side, which], pairs_other[side, which])

    def widen(n):
        at = pl.ds(pl.multiple_of(n * ROWS, ROWS), ROWS)
        for momentum in range(4):
            real = source[momentum // 2, momentum % 2, 0, at, :]
            imag = source[momentum // 2, momentum % 2, 1, at, :]
            wide[momentum, n, :ROWS, :NEV] = real
            wide[momentum, n, :ROWS, NEV:] = -imag
            wide[momentum, n, ROWS:, :NEV] = imag
            wide[momentum, n, ROWS:, NEV:] = real

    def work(targets, n):
        at = pl.ds(pl.multiple_of(n * ROWS, ROWS), ROWS)
        diagonal = (
            lax.broadcasted_iota(jnp.int32, (ROWS, NEV), 0) + n * ROWS
            == lax.broadcasted_iota(jnp.int32, (ROWS, NEV), 1)
        )
        for slot, target, of_group in targets:
            for which in range(PAIRS):
                i = slot * PAIRS + which
                a = pair(of_group, which, 0)
                b = lax.rem(pair(of_group, which, 1), 2)
                full = jnp.dot(
                    wide[a, n], target[b].reshape(2 * NEV, NEV), preferred_element_type=jnp.float32
                )
                real, imag = full[:ROWS], full[ROWS:]
                plus = real + imag
                flipped = (real - imag).T
                box = folded(plus * flips[i, at, :])
                sums[i, at, :] = plus
                flips[i, :, at] = flipped
                boxes[i] += box + folded(sums[i, :, at] * flipped)
                directs[i] += folded(jnp.where(diagonal, real, 0.0))

    fed_group = jnp.where(core == 0, from_left, from_right)
    own_part, near_part = (0, own, group), (1, near, group)
    fed_part, ahead_part = (2, fed, fed_group), (3, ahead, from_right)

    @pl.when(core == 0)
    def _():
        to_left(0, many=nearly).wait_send()

        @pl.loop(0, PIECES)
        def _(j):
            to_relay(j).start()

        spare_copy.wait_recv()
        spare_right.start()

        @pl.loop(0, CHUNKS)
        def _(n):
            to_left(n * SUB, many=SUB).wait_recv()
            feed_ahead(n * SUB, SUB).start()

        feed_source(0, PIECES).wait_recv()
        near_copy.wait_recv()

        @pl.loop(0, CHUNKS)
        def _(n):
            relay_core(n * SUB, SUB).wait_recv()

            @pl.when(n < CHUNKS - 1)
            def _():
                relay_y(n * SUB, SUB).wait_recv()

            @pl.when(n == CHUNKS - 1)
            def _():
                relay_y(last + 1 - SUB, SUB - 1).wait_recv()
                spare_core.wait_recv()

            widen(n)
            work([own_part, near_part, fed_part, ahead_part], n)

    @pl.when(core == 1)
    def _():
        @pl.loop(0, 2 * CHUNKS)
        def _(step):
            for q in range(SUB):

                @pl.when(step < CHUNKS)
                def _():
                    j = step * SUB + q
                    to_right(j).wait_recv()
                    over_y(j).start()
                    feed_source(j).start()

                @pl.when(step >= CHUNKS)
                def _():
                    j = (step - CHUNKS) * SUB + q
                    to_relay(j).wait_recv()
                    relay_core(j).start()

                    @pl.when(j < last)
                    def _():
                        relay_y(j).start()

                if q == 0:

                    @pl.when(step == CHUNKS - 1)
                    def _():
                        to_right(0, many=nearly).wait_send()

                        @pl.loop(0, PIECES)
                        def _(j):
                            to_left(j, sent=2).start()

                if q == 2:

                    @pl.when(step == 1)
                    def _():
                        near_copy.wait_recv()

                    @pl.when((step >= 1) & (step <= CHUNKS))
                    def _():
                        over_y((step - 1) * SUB, SUB).wait_recv()
                        widen(step - 1)
                        work([own_part, near_part], step - 1)

                if q == 0:

                    @pl.when(step == CHUNKS + 1)
                    def _():
                        feed_ahead(0, PIECES).wait_recv()

                    @pl.when((step == CHUNKS + 1) | (step == CHUNKS + 2))
                    def _():
                        @pl.loop(0, CHUNKS // 2)
                        def _(n):
                            work([fed_part], (step - CHUNKS - 1) * (CHUNKS // 2) + n)

        spare_right.wait_recv()
        spare_core.start()

        @pl.loop(0, CHUNKS)
        def _(n):
            to_left(n * SUB, many=SUB).wait_recv()

        for n in range(CHUNKS):
            work([ahead_part], n)

    separations = (1, 2 - 2 * core, 2 * core, 3)
    groups = (group, group, fed_group, from_right)
    lane = lax.broadcasted_iota(jnp.int32, (8, 128), 1)
    sublane = lax.broadcasted_iota(jnp.int32, (8, 128), 0)
    wanted = functools.reduce(
        jnp.add, [jnp.where(lane % SEPS == r, deltas[r], 0) for r in range(SEPS)]
    )
    for slot in range(SEPS):
        for kind, values in enumerate((directs, boxes)):
            for which in range(PAIRS):
                line = slot * 8 + which * 2 + kind
                rows_out[line : line + 1, :] = values[slot * PAIRS + which].sum(0, keepdims=True)
    totals = jnp.broadcast_to(rows_out[...].sum(1, keepdims=True), rows_out.shape)
    placed = functools.reduce(
        jnp.add,
        [
            jnp.where(
                (wanted == separations[slot]) & (lane // SEPS % 2 == groups[slot]) & (lane // (2 * SEPS) == sublane),
                totals[slot * 8 : slot * 8 + 8],
                0.0,
            )
            for slot in range(SEPS)
        ],
    )
    tile[...] = placed.sum(0, keepdims=True)

    returns = [
        remote(tile, back.at[group], stage_sems.at[0], stage_sems.at[1], device) for device in back_devices
    ]
    for copy in returns:
        copy.start()

    def sent():
        @pl.when(core == 0)
        def _():
            to_left(nearly, sent=1, many=PIECES - nearly).wait_send()
            to_relay(0, PIECES).wait_send()
            spare_copy.wait_send()
            spare_right.wait_send()
            feed_ahead(0, PIECES).wait_send()

        @pl.when(core == 1)
        def _():
            to_right(nearly, sent=1, many=PIECES - nearly).wait_send()
            to_left(0, sent=2, many=PIECES).wait_send()
            over_y(0, PIECES).wait_send()
            feed_source(0, PIECES).wait_send()
            relay_y(0, last).wait_send()
            spare_core.wait_send()
            relay_core(0, PIECES).wait_send()

        near_copy.wait_send()
        pair_copy.wait_send()

    def stage(src, held, mine, devices, sems):
        for device in devices:
            remote(src, held.at[mine], stage_sems.at[sems], stage_sems.at[sems + 1], device).start()
        held[mine] = src[...]
        if held is first:
            sent()
        arrived = held.at[: len(devices)]
        all_of_them = remote(arrived, arrived, stage_sems.at[sems], stage_sems.at[sems + 1], devices[0])
        all_of_them.wait_recv()
        return all_of_them, functools.reduce(jnp.add, [held[i] for i in range(held.shape[0])])

    def deliver(values, out):
        for which in range(PAIRS):
            for kind in range(2):
                begin = (which * 2 + kind) * 2 * SEPS
                both_groups = values[:, begin : begin + SEPS], values[:, begin + SEPS : begin + 2 * SEPS]
                results[out, which, kind : kind + 1, :] = jnp.where(group == 0, *both_groups)

    copies_1, value = stage(tile, first, place_in_level, level_devices, 2)
    after_first[...] = value
    copies_2, value = stage(after_first, second, level, column_devices, 4)
    deliver(value, 1)
    both = remote(back, back, stage_sems.at[0], stage_sems.at[1], back_devices[0])
    both.wait_recv()
    deliver(back[0] + back[1], 0)
    for copies in (both, copies_1, copies_2):
        copies.wait_send()


def per_device(fields, mom_pairs, deltas):
    field = (2, 2, NEV, NEV)
    dma = pltpu.SemaphoreType.DMA
    results = pl.pallas_call(
        trace_kernel,
        out_shape=pltpu.VMEM((2, PAIRS, 2, SEPS), jnp.float32),
        in_specs=[
            pl.BlockSpec(memory_space=pl.ANY),
            pl.BlockSpec(memory_space=pl.ANY),
            pl.BlockSpec(memory_space=pl.ANY),
        ],
        out_specs=pl.BlockSpec(memory_space=pltpu.VMEM),
        scratch_shapes=[
            pltpu.VMEM(field, jnp.bfloat16),
            pltpu.VMEM(field, jnp.bfloat16),
            pltpu.VMEM(field, jnp.bfloat16),
            pltpu.VMEM(field, jnp.bfloat16),
            pltpu.VMEM(field, jnp.bfloat16),
            pltpu.VMEM((2, 2, PIECE_ROWS, NEV), jnp.bfloat16),
            pltpu.VMEM((2, 2, PIECE_ROWS, NEV), jnp.bfloat16),
            pltpu.VMEM((2, *field), jnp.bfloat16),
            pltpu.VMEM((4, CHUNKS, 2 * ROWS, 2 * NEV), jnp.bfloat16),
            pltpu.VMEM((SEPS * PAIRS, NEV, NEV), jnp.float32),
            pltpu.VMEM((SEPS * PAIRS, NEV, NEV), jnp.float32),
            pltpu.VMEM((SEPS * PAIRS, 8, 128), jnp.float32),
            pltpu.VMEM((SEPS * PAIRS, 8, 128), jnp.float32),
            pltpu.VMEM((SEPS * 8, 128), jnp.float32),
            pltpu.VMEM((2, PAIRS), jnp.int32),
            pltpu.SMEM((2, PAIRS), jnp.int32),
            pltpu.SMEM((2, PAIRS), jnp.int32),
            pltpu.SMEM((SEPS,), jnp.int32),
            pltpu.VMEM((1, 128), jnp.float32),
            pltpu.VMEM((2, 1, 128), jnp.float32),
            pltpu.VMEM((LEVEL_DEVICES, 1, 128), jnp.float32),
            pltpu.VMEM((LEVELS, 1, 128), jnp.float32),
            pltpu.VMEM((1, 128), jnp.float32),
            dma,
        ]
        + [dma((n,)) for n in (4, 2, 3, 4, PIECES, PIECES, CHUNKS, CHUNKS, CHUNKS, 1, 6, 6)],
        compiler_params=pltpu.CompilerParams(
            collective_id=0, has_side_effects=True, vmem_limit_bytes=62 * 1024 * 1024
        ),
        name="traces",
    )(mom_pairs.T, deltas, fields.reshape(field))
    times, total = results.transpose(0, 2, 3, 1)
    return times[None], total


def solution(mesh):
    return jax.shard_map(
        per_device,
        mesh=mesh,
        in_specs=(P("tm", "mom", None, None, None), P("mom", None), P()),
        out_specs=(P("tm", None, None, "mom"), P(None, None, "mom")),
        check_vma=False,
    )
```

```python
import functools

import jax
import jax.numpy as jnp
from jax import lax
from jax.experimental import pallas as pl
from jax.experimental.pallas import tpu as pltpu
from jax.sharding import PartitionSpec as P

MESH = pl.DeviceIdType.MESH
CHIPS_PER_PLANE = 32
ROWS = 128
CHUNKS = 4
LEVELS, LEVEL_DEVICES = 8, 32
SUB = 4
PIECES = CHUNKS * SUB
PIECE_ROWS = ROWS // SUB
NEV = ROWS * CHUNKS
PAIRS = 3
SEPS = 4


def place():
    time, group = lax.axis_index("tm"), lax.axis_index("mom")
    count = lax.axis_size("tm")
    chip, core = time // 2, time % 2
    swap_right = (chip % CHIPS_PER_PLANE) // (CHIPS_PER_PLANE - 1)
    swap_left = ((chip + 1) % CHIPS_PER_PLANE == 1).astype(jnp.int32)
    right = {"tm": (time + 2) % count, "mom": (group + swap_right) % 2}
    left = {"tm": (time + count - 2) % count, "mom": (group + swap_left) % 2}
    across = {"tm": time, "mom": 1 - group}
    partner = {"tm": time + 1 - 2 * core, "mom": group}
    return time, group, core, right, left, across, partner


def folded(values):
    total = values.reshape(-1, 8, values.shape[-1]).sum(0)
    lanes = [total[:, i : i + 128] for i in range(0, values.shape[-1], 128)]
    return functools.reduce(jnp.add, lanes)


def trace_kernel(
    pairs, deltas_in, fields, results,
    own, near, fed, ahead, relay, spare, relay_spare, source, wide, sums, flips, boxes, directs, rows_out, pairs_in, pairs_own, pairs_other, deltas,
    tile, back, first, second, after_first, load_sem, pair_sems, near_sems, first_sent, passed,
    recv_right, recv_relay, recv_left, recv_y, recv_core, recv_fed, stage_sems, spare_sems,
):
    time, group, core, right, left, across, partner = place()
    count = lax.axis_size("tm")
    from_left = left["mom"]
    from_right = right["mom"]

    def rows(j, count_of=1):
        return pl.ds(pl.multiple_of(j * PIECE_ROWS, PIECE_ROWS), PIECE_ROWS * count_of)

    def remote(src, dst, send, recv, device):
        return pltpu.make_async_remote_copy(
            src_ref=src, dst_ref=dst, send_sem=send, recv_sem=recv, device_id=device, device_id_type=MESH
        )

    def to_right(j, sent=0, many=1):
        at = rows(j, many)
        return remote(
            own.at[:, :, at, :], source.at[group, :, :, at, :], first_sent.at[sent], recv_right.at[j], right
        )

    def to_left(j, sent=0, many=1):
        at = rows(j, many)
        return remote(own.at[:, :, at, :], ahead.at[:, :, at, :], first_sent.at[sent], recv_left.at[j // SUB], left)

    def to_relay(j, many=1):
        at = rows(j, many)
        device = {"tm": (time + 3) % count, "mom": right["mom"]}
        return remote(own.at[:, :, at, :], relay.at[:, :, at, :], first_sent.at[2], recv_relay.at[j], device)

    def relay_y(j, many=1):
        at = rows(j, many)
        device = {"tm": partner["tm"], "mom": 1 - group}
        return remote(
            relay.at[:, :, at, :], source.at[from_left, :, :, at, :], passed.at[0], recv_y.at[j // SUB], device
        )

    def relay_core(j, many=1):
        at = rows(j, many)
        return remote(
            relay.at[:, :, at, :], source.at[from_left, :, :, at, :], passed.at[1], recv_core.at[j // SUB], partner
        )

    def over_y(j, many=1):
        part = source.at[from_left, :, :, rows(j, many), :]
        return remote(part, part, passed.at[2], recv_y.at[j // SUB], across)

    def feed_source(j, many=1):
        at = rows(j, many)
        return remote(source.at[from_left, :, :, at, :], fed.at[:, :, at, :], passed.at[3], recv_fed.at[0], partner)

    def feed_ahead(j, many=1):
        at = rows(j, many)
        return remote(ahead.at[:, :, at, :], fed.at[:, :, at, :], passed.at[3], recv_fed.at[0], partner)

    nearly = PIECES - SUB // 2
    last = PIECES - 1
    spare_copy = remote(own.at[:, :, rows(last), :], spare, spare_sems.at[0], spare_sems.at[1], across)
    spare_right = remote(
        spare, relay_spare, spare_sems.at[2], spare_sems.at[3], {"tm": (time + 3) % count, "mom": right["mom"]}
    )
    spare_core = remote(
        relay_spare, source.at[1 - from_left, :, :, rows(last), :], spare_sems.at[4], spare_sems.at[5], partner
    )
    soon = PIECES - SUB
    near_copy = remote(own, near, near_sems.at[0], near_sems.at[1], partner)
    pair_copy = remote(pairs, pairs_in, pair_sems.at[0], pair_sems.at[1], across)
    load = pltpu.make_async_copy(fields, own, load_sem)

    level = time // 8 % 8
    place_in_level = (time // 64 * 2 + group) * 8 + time % 8
    in_level = [(place_in_level + d) % LEVEL_DEVICES for d in range(1, LEVEL_DEVICES)]
    in_column = [(level + d) % LEVELS for d in range(1, LEVELS)]
    level_devices = [{"tm": n // 16 * 64 + level * 8 + n % 8, "mom": n // 8 % 2} for n in in_level]
    column_devices = [{"tm": time + (n - level) * 8, "mom": group} for n in in_column]
    back_devices = [{"tm": (time + count - 2) % count, "mom": h} for h in range(2)]
    behind_devices = [{"tm": (time + 2) % count, "mom": h} for h in range(2)]

    barrier = pltpu.get_barrier_semaphore()
    relays = [
        {"tm": (time + count + 3 - 6 * core) % count, "mom": jnp.where(core == 0, right["mom"], left["mom"])},
    ]
    greeted = column_devices + level_devices + back_devices + behind_devices + relays
    for device in greeted:
        pl.semaphore_signal(barrier, inc=1, device_id=device, device_id_type=MESH)
    own_tables = [
        pltpu.make_async_copy(pairs, pairs_own, pair_sems.at[2]),
        pltpu.make_async_copy(deltas_in, deltas, pair_sems.at[3]),
    ]
    load.start()
    for copy in own_tables:
        copy.start()
    load.wait()
    pl.semaphore_wait(barrier, len(greeted))

    @pl.when(core == 1)
    def _():
        @pl.loop(0, PIECES)
        def _(j):
            to_right(j, j // soon).start()

    @pl.when(core == 0)
    def _():
        @pl.loop(0, PIECES)
        def _(j):
            to_left(j, j // nearly).start()

        spare_copy.start()

    pair_copy.start()
    near_copy.start()

    @pl.loop(0, SEPS * PAIRS)
    def _(i):
        boxes[i] = jnp.zeros((8, 128), jnp.float32)
        directs[i] = jnp.zeros((8, 128), jnp.float32)

        @pl.loop(0, NEV // 32)
        def _(r):
            at = pl.ds(pl.multiple_of(r * 32, 32), 32)
            sums[i, at, :] = jnp.zeros((32, NEV), jnp.float32)
            flips[i, at, :] = jnp.zeros((32, NEV), jnp.float32)

    rows_out[...] = jnp.zeros_like(rows_out)
    for copy in own_tables:
        copy.wait()
    pair_copy.wait_recv()
    pair_load = pltpu.make_async_copy(pairs_in, pairs_other, load_sem)
    pair_load.start()
    pair_load.wait()

    def pair(of_group, which, side):
        return jnp.where(of_group == group, pairs_own[side, which], pairs_other[side, which])

    def widen(n):
        at = pl.ds(pl.multiple_of(n * ROWS, ROWS), ROWS)
        for momentum in range(4):
            real = source[momentum // 2, momentum % 2, 0, at, :]
            imag = source[momentum // 2, momentum % 2, 1, at, :]
            wide[momentum, n, :ROWS, :NEV] = real
            wide[momentum, n, :ROWS, NEV:] = -imag
            wide[momentum, n, ROWS:, :NEV] = imag
            wide[momentum, n, ROWS:, NEV:] = real

    def work(targets, n):
        at = pl.ds(pl.multiple_of(n * ROWS, ROWS), ROWS)
        diagonal = (
            lax.broadcasted_iota(jnp.int32, (ROWS, NEV), 0) + n * ROWS
            == lax.broadcasted_iota(jnp.int32, (ROWS, NEV), 1)
        )
        for slot, target, of_group in targets:
            for which in range(PAIRS):
                i = slot * PAIRS + which
                a = pair(of_group, which, 0)
                b = lax.rem(pair(of_group, which, 1), 2)
                full = jnp.dot(
                    wide[a, n], target[b].reshape(2 * NEV, NEV), preferred_element_type=jnp.float32
                )
                real, imag = full[:ROWS], full[ROWS:]
                plus = real + imag
                flipped = (real - imag).T
                box = folded(plus * flips[i, at, :])
                sums[i, at, :] = plus
                flips[i, :, at] = flipped
                boxes[i] += box + folded(sums[i, :, at] * flipped)
                directs[i] += folded(jnp.where(diagonal, real, 0.0))

    fed_group = jnp.where(core == 0, from_left, from_right)
    own_part, near_part = (0, own, group), (1, near, group)
    fed_part, ahead_part = (2, fed, fed_group), (3, ahead, from_right)

    @pl.when(core == 0)
    def _():
        to_left(0, many=nearly).wait_send()

        @pl.loop(0, PIECES)
        def _(j):
            to_relay(j).start()

        spare_copy.wait_recv()
        spare_right.start()

        @pl.loop(0, CHUNKS)
        def _(n):
            to_left(n * SUB, many=SUB).wait_recv()
            feed_ahead(n * SUB, SUB).start()

        feed_source(0, PIECES).wait_recv()
        near_copy.wait_recv()

        @pl.loop(0, CHUNKS)
        def _(n):
            relay_core(n * SUB, SUB).wait_recv()

            @pl.when(n < CHUNKS - 1)
            def _():
                relay_y(n * SUB, SUB).wait_recv()

            @pl.when(n == CHUNKS - 1)
            def _():
                relay_y(last + 1 - SUB, SUB - 1).wait_recv()
                spare_core.wait_recv()

            widen(n)
            work([own_part, near_part, fed_part, ahead_part], n)

    @pl.when(core == 1)
    def _():
        @pl.loop(0, 2 * CHUNKS)
        def _(step):
            for q in range(SUB):

                @pl.when(step < CHUNKS)
                def _():
                    j = step * SUB + q
                    to_right(j).wait_recv()
                    over_y(j).start()
                    feed_source(j).start()

                @pl.when(step >= CHUNKS)
                def _():
                    j = (step - CHUNKS) * SUB + q
                    to_relay(j).wait_recv()
                    relay_core(j).start()

                    @pl.when(j < last)
                    def _():
                        relay_y(j).start()

                if q == 0:

                    @pl.when(step == CHUNKS - 1)
                    def _():
                        to_right(0, many=soon).wait_send()

                        @pl.loop(0, PIECES)
                        def _(j):
                            to_left(j, sent=2).start()

                if q == 2:

                    @pl.when(step == 1)
                    def _():
                        near_copy.wait_recv()

                    @pl.when((step >= 1) & (step <= CHUNKS))
                    def _():
                        over_y((step - 1) * SUB, SUB).wait_recv()
                        widen(step - 1)
                        work([own_part, near_part], step - 1)

                if q == 0:

                    @pl.when(step == CHUNKS + 1)
                    def _():
                        feed_ahead(0, PIECES).wait_recv()

                    @pl.when((step == CHUNKS + 1) | (step == CHUNKS + 2))
                    def _():
                        @pl.loop(0, CHUNKS // 2)
                        def _(n):
                            work([fed_part], (step - CHUNKS - 1) * (CHUNKS // 2) + n)

        spare_right.wait_recv()
        spare_core.start()

        @pl.loop(0, CHUNKS)
        def _(n):
            to_left(n * SUB, many=SUB).wait_recv()

        for n in range(CHUNKS):
            work([ahead_part], n)

    separations = (1, 2 - 2 * core, 2 * core, 3)
    groups = (group, group, fed_group, from_right)
    lane = lax.broadcasted_iota(jnp.int32, (8, 128), 1)
    sublane = lax.broadcasted_iota(jnp.int32, (8, 128), 0)
    wanted = functools.reduce(
        jnp.add, [jnp.where(lane % SEPS == r, deltas[r], 0) for r in range(SEPS)]
    )
    for slot in range(SEPS):
        for kind, values in enumerate((directs, boxes)):
            for which in range(PAIRS):
                line = slot * 8 + which * 2 + kind
                rows_out[line : line + 1, :] = values[slot * PAIRS + which].sum(0, keepdims=True)
    totals = jnp.broadcast_to(rows_out[...].sum(1, keepdims=True), rows_out.shape)
    placed = functools.reduce(
        jnp.add,
        [
            jnp.where(
                (wanted == separations[slot]) & (lane // SEPS % 2 == groups[slot]) & (lane // (2 * SEPS) == sublane),
                totals[slot * 8 : slot * 8 + 8],
                0.0,
            )
            for slot in range(SEPS)
        ],
    )
    tile[...] = placed.sum(0, keepdims=True)

    returns = [
        remote(tile, back.at[group], stage_sems.at[0], stage_sems.at[1], device) for device in back_devices
    ]
    for copy in returns:
        copy.start()

    def sent():
        @pl.when(core == 0)
        def _():
            to_left(nearly, sent=1, many=PIECES - nearly).wait_send()
            to_relay(0, PIECES).wait_send()
            spare_copy.wait_send()
            spare_right.wait_send()
            feed_ahead(0, PIECES).wait_send()

        @pl.when(core == 1)
        def _():
            to_right(soon, sent=1, many=PIECES - soon).wait_send()
            to_left(0, sent=2, many=PIECES).wait_send()
            over_y(0, PIECES).wait_send()
            feed_source(0, PIECES).wait_send()
            relay_y(0, last).wait_send()
            spare_core.wait_send()
            relay_core(0, PIECES).wait_send()

        near_copy.wait_send()
        pair_copy.wait_send()

    def stage(src, held, mine, devices, sems):
        for device in devices:
            remote(src, held.at[mine], stage_sems.at[sems], stage_sems.at[sems + 1], device).start()
        held[mine] = src[...]
        if held is first:
            sent()
        arrived = held.at[: len(devices)]
        all_of_them = remote(arrived, arrived, stage_sems.at[sems], stage_sems.at[sems + 1], devices[0])
        all_of_them.wait_recv()
        return all_of_them, functools.reduce(jnp.add, [held[i] for i in range(held.shape[0])])

    def deliver(values, out):
        for which in range(PAIRS):
            for kind in range(2):
                begin = (which * 2 + kind) * 2 * SEPS
                both_groups = values[:, begin : begin + SEPS], values[:, begin + SEPS : begin + 2 * SEPS]
                results[out, which, kind : kind + 1, :] = jnp.where(group == 0, *both_groups)

    copies_1, value = stage(tile, first, place_in_level, level_devices, 2)
    after_first[...] = value
    copies_2, value = stage(after_first, second, level, column_devices, 4)
    deliver(value, 1)
    both = remote(back, back, stage_sems.at[0], stage_sems.at[1], back_devices[0])
    both.wait_recv()
    deliver(back[0] + back[1], 0)
    for copies in (both, copies_1, copies_2):
        copies.wait_send()


def per_device(fields, mom_pairs, deltas):
    field = (2, 2, NEV, NEV)
    dma = pltpu.SemaphoreType.DMA
    results = pl.pallas_call(
        trace_kernel,
        out_shape=pltpu.VMEM((2, PAIRS, 2, SEPS), jnp.float32),
        in_specs=[
            pl.BlockSpec(memory_space=pl.ANY),
            pl.BlockSpec(memory_space=pl.ANY),
            pl.BlockSpec(memory_space=pl.ANY),
        ],
        out_specs=pl.BlockSpec(memory_space=pltpu.VMEM),
        scratch_shapes=[
            pltpu.VMEM(field, jnp.bfloat16),
            pltpu.VMEM(field, jnp.bfloat16),
            pltpu.VMEM(field, jnp.bfloat16),
            pltpu.VMEM(field, jnp.bfloat16),
            pltpu.VMEM(field, jnp.bfloat16),
            pltpu.VMEM((2, 2, PIECE_ROWS, NEV), jnp.bfloat16),
            pltpu.VMEM((2, 2, PIECE_ROWS, NEV), jnp.bfloat16),
            pltpu.VMEM((2, *field), jnp.bfloat16),
            pltpu.VMEM((4, CHUNKS, 2 * ROWS, 2 * NEV), jnp.bfloat16),
            pltpu.VMEM((SEPS * PAIRS, NEV, NEV), jnp.float32),
            pltpu.VMEM((SEPS * PAIRS, NEV, NEV), jnp.float32),
            pltpu.VMEM((SEPS * PAIRS, 8, 128), jnp.float32),
            pltpu.VMEM((SEPS * PAIRS, 8, 128), jnp.float32),
            pltpu.VMEM((SEPS * 8, 128), jnp.float32),
            pltpu.VMEM((2, PAIRS), jnp.int32),
            pltpu.SMEM((2, PAIRS), jnp.int32),
            pltpu.SMEM((2, PAIRS), jnp.int32),
            pltpu.SMEM((SEPS,), jnp.int32),
            pltpu.VMEM((1, 128), jnp.float32),
            pltpu.VMEM((2, 1, 128), jnp.float32),
            pltpu.VMEM((LEVEL_DEVICES, 1, 128), jnp.float32),
            pltpu.VMEM((LEVELS, 1, 128), jnp.float32),
            pltpu.VMEM((1, 128), jnp.float32),
            dma,
        ]
        + [dma((n,)) for n in (4, 2, 3, 4, PIECES, PIECES, CHUNKS, CHUNKS, CHUNKS, 1, 6, 6)],
        compiler_params=pltpu.CompilerParams(
            collective_id=0, has_side_effects=True, vmem_limit_bytes=62 * 1024 * 1024
        ),
        name="traces",
    )(mom_pairs.T, deltas, fields.reshape(field))
    times, total = results.transpose(0, 2, 3, 1)
    return times[None], total


def solution(mesh):
    return jax.shard_map(
        per_device,
        mesh=mesh,
        in_specs=(P("tm", "mom", None, None, None), P("mom", None), P()),
        out_specs=(P("tm", None, None, "mom"), P(None, None, "mom")),
        check_vma=False,
    )
```
